32 devices in a mesh: groups: 2 (over x), ep: 4 (over y, core), rep: 4 (over z).
Axes of the slice: x: 2, y: 2, z: 4, core: 2. Of those that a mesh axis runs over, the one named last changes fastest.
Arguments:
- prompt_hidden: bfloat16 [8, 96, 2048], P('groups', 'ep'), parts along dimension 0, may hold values from -6 to 6
- decode_hidden: bfloat16 [64, 8, 2048], P(('groups', 'ep'), 'rep'), parts along dimension 0, may hold values from -6 to 6
- queries: bfloat16 [64, 8, 2048], P(('groups', 'ep'), None, 'rep'), parts along dimension 0, may hold values from -128 to 128
- attn_gain: float32 [2048], replicated, may hold values from 0.1 to 1.9
- key_value_weight: bfloat16 [2048, 1024], P(None, 'rep'), may hold values from -0.125 to 0.125
- out_weight: bfloat16 [2048, 2048], P('rep'), may hold values from -0.5 to 0.5
- moe_gain: float32 [2048], replicated, may hold values from 0.1 to 1.9
- gate_weight: bfloat16 [16, 2048, 768], P(('ep', 'rep')), may hold values from -0.125 to 0.125
- up_weight: bfloat16 [16, 2048, 768], P(('ep', 'rep')), may hold values from -0.125 to 0.125
- down_weight: bfloat16 [16, 768, 2048], P(('ep', 'rep')), may hold values from -0.21875 to 0.21875
- expert_table: int32 [151936], replicated, may hold values from 0 to 15, as said below
- token_ids: int32 [32, 8], P('ep', 'rep'), may hold values from 0 to 151935, as said below
- prompt_lengths: int32 [8], P('groups'), parts along dimension 0, may hold values from 1 to 96, 240 in all
Outputs:
- layer_out: bfloat16 [64, 8, 2048], P(('groups', 'ep'), 'rep'), parts along dimension 0
The draws below stay inside these ranges and needn't reach their ends.
There are 2 independent parts, one for each index of `groups`. The reference program is written for one: setup_inputs(seed, part) draws one part's arguments, and reference() takes and returns one part's arrays. A program takes and returns all parts, laid end to end along the dimension named above; an argument that names none is the same for every part. Nothing has to cross between parts.
Inputs may be any that keep to these rules, and one draw needn't show every extreme that they name: `expert_table`: each expert is the value of exactly 9496 entries. `token_ids`: a device holds the 8 sequences of its index of ep at 8 // 4 steps of its index of rep; of these tokens at most 2 go to one expert; in every draw one expert receives exactly 2 from every device. `prompt_lengths`: the lengths of a group sum to 240 and the longest is 96.
All inputs are finite; a program needn't handle non-finite values.
Results may differ from the reference program's by a relative error of at most 0.017.
The reference program's roundings to bfloat16 on the way count: a program that leaves them out, or rounds other values in their place, can miss the bound.
Values may be sent and summed in bfloat16 or wider, within the bound.
No kernel may reach another device: no remote copies, remote signals or barrier semaphores. Data moves between devices by JAX's collectives and lax.ppermute only.
A program may use at most 128 MiB of HBM per device.

```python
import math
import jax
import jax.numpy as jnp
import numpy as np
from jax import lax

MODEL_DIM = 2048
FF = 768
HEAD_DIM = 128
QUERY_HEADS = 16
KEY_VALUE_HEADS = 4
VOCAB = 151936
GROUP_PROMPTS = 4
PLEN = 96
DECODE_COUNT = 8
CAP = 2
SEQ_DEV = 8
SEQS = 32
EXPERTS = 16
N_EP = 4
N_REP = 4


def hash_order(key):
    return jax.random.permutation(jax.random.fold_in(key, 7), VOCAB).astype(jnp.int32)


def draw_expert_table(key, part):
    return (hash_order(key) % EXPERTS).astype(jnp.int32)


def draw_token_ids(key, part):
    hash_perm = hash_order(key)
    inverse = jnp.zeros((VOCAB,), jnp.int32).at[hash_perm].set(jnp.arange(VOCAB, dtype=jnp.int32))
    ep_count = SEQS // SEQ_DEV
    rep_count = EXPERTS // ep_count
    step_rows = DECODE_COUNT // rep_count
    row_count = SEQ_DEV * step_rows
    blocks = EXPERTS
    slot_cols = EXPERTS * CAP
    key_hot, key_pick, key_place, key_token = jax.random.split(jax.random.fold_in(key, 13), 4)
    hot_expert = jax.random.randint(key_hot, (), 0, EXPERTS, dtype=jnp.int32)
    columns = jnp.arange(slot_cols, dtype=jnp.int32)
    column_expert = (columns // CAP).astype(jnp.int32)
    scores = jax.random.randint(key_pick, (blocks, slot_cols), 0, 1 << 20, dtype=jnp.int32) * slot_cols + columns[None, :]
    scores = jnp.where(column_expert[None, :] == hot_expert, 1 << 30, scores)
    picked_cols = lax.top_k(scores, row_count)[1].astype(jnp.int32)
    experts = jnp.take(column_expert, picked_cols)
    place_score = jax.random.randint(key_place, (blocks, row_count), 0, 1 << 20, dtype=jnp.int32) * row_count + jnp.arange(row_count, dtype=jnp.int32)[None, :]
    row_order = jnp.argsort(place_score, axis=1).astype(jnp.int32)
    experts = jnp.take_along_axis(experts, row_order, axis=1)
    within = jax.random.randint(key_token, (blocks, row_count), 0, VOCAB // EXPERTS, dtype=jnp.int32)
    token_rows = jnp.take(inverse, experts + EXPERTS * within)
    token_rows = token_rows.reshape(ep_count, rep_count, SEQ_DEV, step_rows).transpose(0, 2, 1, 3)
    return token_rows.reshape(SEQS, DECODE_COUNT).astype(jnp.int32)


def draw_queries(key, part):
    base_draw = jnp.clip(jax.random.normal(key, (SEQS, DECODE_COUNT, QUERY_HEADS, HEAD_DIM), jnp.float32), -4.0, 4.0)
    return base_draw.reshape(SEQS, DECODE_COUNT, QUERY_HEADS * HEAD_DIM).astype(jnp.bfloat16)


def levels(own_key, dims, cuts, low, top_value):
    def one(position, shards_of):
        steps = jax.random.uniform(jax.random.fold_in(jax.random.fold_in(own_key, 6), position), (shards_of,), jnp.float32, low / len(cuts), top_value / len(cuts))
        return jnp.repeat(jnp.exp(steps), dims[position] // shards_of).reshape((-1,) + (1,) * (len(dims) - position - 1))

    gain = one(*cuts[0])
    for cut in cuts[1:]:
        gain = gain * one(*cut)
    return gain


def profile(count, total, bound, skew):
    loads = [(1 << 20) // math.isqrt(standing ** skew) + 1 for standing in range(2, count + 1)]
    spare, holding = total - bound - (count - 1), [1] * (count - 1)
    while spare > 0:
        movable = [i for i in range(count - 1) if holding[i] < bound]
        whole, left = sum([loads[i] for i in movable]), spare
        for i in movable:
            addition = min(bound - holding[i], max(1, left * loads[i] // whole), spare)
            holding[i] = holding[i] + addition
            spare = spare - addition
    return np.array([bound] + holding)


def uneven_parts(rng, count, total, reach, skew):
    if count == 2:
        one = jax.random.randint(rng, (), max(1, total - reach), min(reach, total - 1) + 1)
        return jnp.stack([one, total - one])
    sizes = jnp.asarray(profile(count, total, reach, skew), jnp.int32)
    couples = (count - 1) // 2
    donor, sink = sizes[1:1 + 2 * couples:2], sizes[2:2 + 2 * couples:2]
    margin = jnp.minimum(donor - 1, reach - sink)
    moved = jax.random.randint(jax.random.fold_in(rng, 1), (couples,), 0, 1 << 20) % (margin + 1)
    sizes = sizes.at[1:1 + 2 * couples:2].set(donor - moved).at[2:2 + 2 * couples:2].set(sink + moved)
    return sizes[jax.random.permutation(jax.random.fold_in(rng, 2), count)]


def bell_draw(own_key, shape, deviation, reach, cuts=(), kind=jnp.bfloat16):
    gain = levels(own_key, shape, cuts, -0.22, 0.18) if cuts else 1.0
    values = jax.random.normal(own_key, shape, jnp.float32) * deviation * gain
    return jnp.minimum(jnp.maximum(values, -reach), reach).astype(kind)


def setup_inputs(seed: int = 0, part: int = 0) -> dict:
    key_of = jax.random.split(jax.random.key(seed), 14)
    part_splits = jax.random.split(jax.random.fold_in(key_of[13], part), 14)
    prompt_hidden = bell_draw(part_splits[0], (GROUP_PROMPTS, PLEN, MODEL_DIM), 1.0, 6.0, ((1, 4),))
    decode_hidden = bell_draw(part_splits[1], (SEQS, DECODE_COUNT, MODEL_DIM), 1.0, 6.0, ((0, 4), (1, 4)))
    queries = draw_queries(jax.random.fold_in(jax.random.fold_in(key_of[13], part), 71), part)
    attn_gain = jnp.clip(1.0 + 0.18 * jax.random.normal(key_of[3], (MODEL_DIM,), jnp.float32), 0.1, 1.9)
    key_value_weight = bell_draw(key_of[4], (MODEL_DIM, KEY_VALUE_HEADS * 2 * HEAD_DIM), MODEL_DIM ** -0.5, 0.125, ((1, 4),))
    out_weight = bell_draw(key_of[5], (QUERY_HEADS * HEAD_DIM, MODEL_DIM), (QUERY_HEADS * HEAD_DIM // 16) ** -0.5, 0.5, ((0, 4),))
    moe_gain = jnp.clip(1.0 + 0.18 * jax.random.normal(key_of[6], (MODEL_DIM,), jnp.float32), 0.1, 1.9)
    gate_weight = bell_draw(key_of[7], (EXPERTS, MODEL_DIM, FF), MODEL_DIM ** -0.5, 0.125, ((0, 16),))
    up_weight = bell_draw(key_of[8], (EXPERTS, MODEL_DIM, FF), MODEL_DIM ** -0.5, 0.125, ((0, 16),))
    down_weight = bell_draw(key_of[9], (EXPERTS, FF, MODEL_DIM), FF ** -0.5, 0.21875, ((0, 16),))
    expert_table = draw_expert_table(jax.random.fold_in(key_of[13], 71), part)
    token_ids = draw_token_ids(jax.random.fold_in(key_of[13], 71), part)
    prompt_lengths = uneven_parts(part_splits[12], GROUP_PROMPTS, 5 * PLEN // 2, PLEN, 1).astype(jnp.int32)
    return dict(prompt_hidden=prompt_hidden, decode_hidden=decode_hidden, queries=queries, attn_gain=attn_gain, key_value_weight=key_value_weight, out_weight=out_weight, moe_gain=moe_gain, gate_weight=gate_weight, up_weight=up_weight, down_weight=down_weight, expert_table=expert_table, token_ids=token_ids, prompt_lengths=prompt_lengths)


EPS = 1e-06
THETA = 1000000.0

def rms_scale(hidden, gain_vec):
    widened = hidden.astype(jnp.float32)
    mean_sq = lax.optimization_barrier(jnp.mean(widened * widened, axis=-1, keepdims=True))
    return widened * lax.rsqrt(mean_sq + EPS) * gain_vec

def rotate(vectors, positions):
    half_dim = vectors.shape[-1] // 2
    inverse_freq = jnp.exp(jnp.arange(half_dim, dtype=jnp.float32) * (-2.0 * math.log(THETA) / vectors.shape[-1]))
    angles = positions[..., None] * inverse_freq
    cosine = jnp.cos(angles)
    sine_part = jnp.sin(angles)
    first_half = vectors[..., :half_dim]
    second_half = vectors[..., half_dim:]
    return jnp.concatenate([first_half * cosine - second_half * sine_part, second_half * cosine + first_half * sine_part], axis=-1)

def project_kv(hidden, gain_vec, key_value_weight, positions):
    leading = hidden.shape[:-1]
    normed = rms_scale(hidden, gain_vec).astype(jnp.bfloat16)
    kv_pairs = jnp.dot(normed.reshape(-1, hidden.shape[-1]), key_value_weight, preferred_element_type=jnp.float32)
    kv_pairs = kv_pairs.reshape(leading + (key_value_weight.shape[1] // (2 * HEAD_DIM), 2, HEAD_DIM))
    key_part = rotate(kv_pairs[..., 0, :], positions[..., None]).astype(jnp.bfloat16)
    value_part = kv_pairs[..., 1, :].astype(jnp.bfloat16)
    return (key_part, value_part)

def reference(prompt_hidden, decode_hidden, queries, attn_gain, key_value_weight, out_weight, moe_gain, gate_weight, up_weight, down_weight, expert_table, token_ids, prompt_lengths):
    samples = SEQS // GROUP_PROMPTS
    prompt_pos = jnp.broadcast_to(jnp.arange(PLEN, dtype=jnp.float32)[None, :], (GROUP_PROMPTS, PLEN))
    prompt_keys, prompt_values = project_kv(prompt_hidden, attn_gain, key_value_weight, prompt_pos)
    prompt_of = (jnp.arange(SEQS, dtype=jnp.int32) // samples).astype(jnp.int32)
    lengths = jnp.take(prompt_lengths, prompt_of)
    decode_pos = lengths[:, None].astype(jnp.float32) + jnp.arange(DECODE_COUNT, dtype=jnp.float32)[None, :]
    decode_keys, decode_values = project_kv(decode_hidden, attn_gain, key_value_weight, decode_pos)
    group_count = QUERY_HEADS // KEY_VALUE_HEADS
    score_scale = HEAD_DIM ** (-0.5)
    key_pos = jnp.arange(PLEN, dtype=jnp.int32)
    causal = jnp.arange(DECODE_COUNT)[None, :] <= jnp.arange(DECODE_COUNT)[:, None]
    self_mask = causal[:, None, None, :]

    def attend(sequence_index):
        query_matrix = queries[sequence_index].astype(jnp.float32).reshape(DECODE_COUNT, KEY_VALUE_HEADS, group_count, HEAD_DIM)
        prompt = prompt_of[sequence_index]
        cache_keys = prompt_keys[prompt].astype(jnp.float32)
        cache_values = prompt_values[prompt].astype(jnp.float32)
        key_valid = key_pos < lengths[sequence_index]
        cache_scores = jnp.einsum('tkgd,nkd->tkgn', query_matrix, cache_keys) * score_scale
        self_scores = jnp.einsum('tkgd,ukd->tkgu', query_matrix, decode_keys[sequence_index].astype(jnp.float32)) * score_scale
        cache_scores = jnp.where(key_valid, cache_scores, -1e+30)
        self_scores = jnp.where(self_mask, self_scores, -1e+30)
        row_top = jnp.maximum(lax.optimization_barrier(jnp.max(cache_scores, axis=-1)), lax.optimization_barrier(jnp.max(self_scores, axis=-1)))
        cache_weights = jnp.where(key_valid, jnp.exp(cache_scores - row_top[..., None]), 0.0)
        self_weights = jnp.where(self_mask, jnp.exp(self_scores - row_top[..., None]), 0.0)
        row_total = lax.optimization_barrier(jnp.sum(cache_weights, axis=-1)) + lax.optimization_barrier(jnp.sum(self_weights, axis=-1))
        numerator = jnp.einsum('tkgn,nkd->tkgd', cache_weights.astype(jnp.bfloat16).astype(jnp.float32), cache_values)
        numerator = numerator + jnp.einsum('tkgu,ukd->tkgd', self_weights.astype(jnp.bfloat16).astype(jnp.float32), decode_values[sequence_index].astype(jnp.float32))
        return (numerator / row_total[..., None]).reshape(DECODE_COUNT, QUERY_HEADS * HEAD_DIM).astype(jnp.bfloat16)
    attended = lax.map(attend, jnp.arange(SEQS, dtype=jnp.int32))
    projected = jnp.dot(attended.reshape(SEQS * DECODE_COUNT, QUERY_HEADS * HEAD_DIM), out_weight, preferred_element_type=jnp.float32).reshape(SEQS, DECODE_COUNT, MODEL_DIM)
    attn_mixed = (decode_hidden.astype(jnp.float32) + projected).astype(jnp.bfloat16)
    normed = rms_scale(attn_mixed, moe_gain).astype(jnp.bfloat16).reshape(SEQS * DECODE_COUNT, MODEL_DIM)
    chosen = jnp.take(expert_table, token_ids.reshape(-1)).astype(jnp.int32)
    row_total_count = SEQS * DECODE_COUNT
    per_expert = CAP * N_EP * N_REP

    def run_expert(collected, expert):
        row_index = jnp.nonzero(chosen == expert, size=per_expert, fill_value=row_total_count)[0].astype(jnp.int32)
        token_rows = jnp.take(normed, row_index, axis=0, mode='fill', fill_value=0)
        gate_proj = jnp.dot(token_rows, gate_weight[expert], preferred_element_type=jnp.float32)
        up_proj = jnp.dot(token_rows, up_weight[expert], preferred_element_type=jnp.float32)
        hidden = (jax.nn.silu(gate_proj) * up_proj).astype(jnp.bfloat16)
        result = jnp.dot(hidden, down_weight[expert], preferred_element_type=jnp.float32).astype(jnp.bfloat16)
        return (collected.at[row_index].set(result, mode='drop'), None)
    expert_out, unused = lax.scan(run_expert, jnp.zeros((row_total_count, MODEL_DIM), jnp.bfloat16), jnp.arange(EXPERTS, dtype=jnp.int32))
    layer_out = (attn_mixed.astype(jnp.float32) + expert_out.astype(jnp.float32).reshape(SEQS, DECODE_COUNT, MODEL_DIM)).astype(jnp.bfloat16)
    return layer_out
```

```python
import math

import jax
import jax.numpy as jnp
from jax import lax
from jax.sharding import PartitionSpec as P

HEAD_DIM = 128
QUERY_HEADS = 16
KEY_VALUE_HEADS = 4
GROUP_PROMPTS = 4
CAP = 2

EPS = 1e-06
THETA = 1000000.0


def partner(index, step, count):
    if count & (count - 1) == 0:
        return index ^ step
    return (count + step - index) % count


def swap(block, axis, step):
    count = lax.axis_size(axis)
    return lax.ppermute(block, axis, [(i, partner(i, step, count)) for i in range(count)])


def normed_of(hidden, gain_vec):
    widened = hidden.astype(jnp.float32)
    mean_sq = jnp.mean(widened * widened, axis=-1, keepdims=True)
    return (widened * lax.rsqrt(mean_sq + EPS) * gain_vec).astype(jnp.bfloat16)


def key_value(hidden, gain_vec, key_value_weight, positions, is_key):
    rows = hidden.shape[0]
    projected = jnp.dot(
        normed_of(hidden, gain_vec), key_value_weight, preferred_element_type=jnp.float32
    )
    half = HEAD_DIM // 2
    freq = jnp.exp(jnp.arange(half, dtype=jnp.float32) * (-2.0 * math.log(THETA) / HEAD_DIM))
    angles = positions[:, None] * freq
    cosine, sine = jnp.cos(angles), jnp.sin(angles)
    out = []
    for b in range(key_value_weight.shape[1] // HEAD_DIM):
        block = projected[:, b * HEAD_DIM : (b + 1) * HEAD_DIM]
        if is_key[b] is not False:
            first, second = block[:, :half], block[:, half:]
            turned = jnp.concatenate(
                [first * cosine - second * sine, second * cosine + first * sine], axis=1
            )
            block = turned if is_key[b] is True else jnp.where(is_key[b], turned, block)
        out.append(block.astype(jnp.bfloat16))
    return jnp.concatenate(out, axis=1) if len(out) > 1 else out[0]


def local(
    prompt_hidden,
    decode_hidden,
    queries,
    attn_gain,
    key_value_weight,
    out_weight,
    moe_gain,
    gate_weight,
    up_weight,
    down_weight,
    expert_table,
    token_ids,
    prompt_lengths,
):
    seqs, step_rows, model_width = decode_hidden.shape
    prompt_len_local = prompt_hidden.shape[1]
    steps_total = queries.shape[1]
    qh_dev = queries.shape[2] // HEAD_DIM
    ep_count, rep_count = lax.axis_size("ep"), lax.axis_size("rep")
    ep_index, rep_index = lax.axis_index("ep"), lax.axis_index("rep")
    samples = seqs * ep_count // GROUP_PROMPTS
    blocks = key_value_weight.shape[1] // HEAD_DIM
    row_count = seqs * step_rows
    own_prompts = max(1, seqs // samples)

    own_rows = decode_hidden.reshape(row_count, model_width)
    others = [swap(own_rows, "rep", k) for k in range(1, rep_count)]
    owners = [partner(rep_index, k, rep_count) for k in range(rep_count)]

    if blocks == 1:
        is_key = [rep_index % 2 == 0]
    else:
        is_key = [b % 2 == 0 for b in range(blocks)]
    heads_here = max(1, blocks // 2)

    prompt_pos = (
        ep_index * prompt_len_local + jnp.arange(prompt_len_local, dtype=jnp.int32)
    ).astype(jnp.float32)
    prompt_part = key_value(
        prompt_hidden.reshape(-1, model_width),
        attn_gain,
        key_value_weight,
        jnp.tile(prompt_pos, GROUP_PROMPTS),
        is_key,
    ).reshape(GROUP_PROMPTS, prompt_len_local, blocks * HEAD_DIM)

    def first_prompt(ep):
        return ep * seqs // samples

    pieces, piece_pos = [], []
    for k in range(ep_count):
        other = partner(ep_index, k, ep_count)
        part = lax.dynamic_slice_in_dim(prompt_part, first_prompt(other), own_prompts, 0)
        pieces.append(swap(part, "ep", k) if k else part)
        piece_pos.append(other * prompt_len_local + jnp.arange(prompt_len_local, dtype=jnp.int32))
    prompt_kv = jnp.concatenate(pieces, axis=1)
    key_pos = jnp.concatenate(piece_pos)

    own_first = first_prompt(ep_index)
    own_lengths = lax.dynamic_slice_in_dim(prompt_lengths, own_first, own_prompts, 0)
    seq_lengths = jnp.repeat(own_lengths, seqs // own_prompts)

    def decode_part(k, hidden):
        step = owners[k] * step_rows + jnp.arange(step_rows, dtype=jnp.int32)
        position = (seq_lengths[:, None] + step[None, :]).astype(jnp.float32).reshape(-1)
        return position

    positions = [decode_part(k, None) for k in range(rep_count)]
    decode_own = key_value(own_rows, attn_gain, key_value_weight, positions[0], is_key)
    decode_rest = key_value(
        jnp.concatenate(others, axis=0),
        attn_gain,
        key_value_weight,
        jnp.concatenate(positions[1:]),
        is_key,
    )
    decode_kv = jnp.concatenate([decode_own, decode_rest], axis=0)
    if blocks == 1:
        partner_prompt, partner_decode = swap((prompt_kv, decode_kv), "rep", 1)
        holds_key = rep_index % 2 == 0

        def both(mine, theirs):
            return jnp.where(
                holds_key,
                jnp.concatenate([mine, theirs], axis=-1),
                jnp.concatenate([theirs, mine], axis=-1),
            )

        prompt_kv, decode_kv = both(prompt_kv, partner_prompt), both(decode_kv, partner_decode)

    tile = min(seqs // own_prompts, 8)
    tiles = seqs // own_prompts // tile
    group = qh_dev // heads_here
    by_owner = jnp.concatenate(
        [lax.dynamic_slice_in_dim(queries, o * step_rows, step_rows, 1)[None] for o in owners]
    )
    tokens = rep_count * tile * step_rows

    def tiled(rows):
        width = rows.shape[-1]
        rows = rows.reshape(rep_count, own_prompts, tiles, tile * step_rows, width)
        return rows.transpose(1, 2, 0, 3, 4).reshape(own_prompts, tiles, tokens, width)

    query_rows = tiled(by_owner.reshape(rep_count, row_count, qh_dev * HEAD_DIM))
    decode_rows = tiled(decode_kv.reshape(rep_count, row_count, -1))
    row_step = jnp.concatenate(
        [
            jnp.tile(o * step_rows + jnp.arange(step_rows, dtype=jnp.int32), tile)
            for o in owners
        ]
    )
    row_seq = jnp.tile(jnp.repeat(jnp.arange(tile, dtype=jnp.int32), step_rows), rep_count)
    self_mask = (row_seq[:, None] == row_seq[None, :]) & (row_step[None, :] <= row_step[:, None])
    prompt_mask = key_pos[None, :] < own_lengths[:, None]
    score_scale = HEAD_DIM ** (-0.5)

    heads = []
    for h in range(heads_here):
        lo = 2 * h * HEAD_DIM
        prompt_keys = prompt_kv[..., lo : lo + HEAD_DIM]
        prompt_values = prompt_kv[..., lo + HEAD_DIM : lo + 2 * HEAD_DIM]
        self_keys = decode_rows[..., lo : lo + HEAD_DIM]
        self_values = decode_rows[..., lo + HEAD_DIM : lo + 2 * HEAD_DIM]
        query = jnp.stack(
            [
                query_rows[..., (h * group + g) * HEAD_DIM : (h * group + g + 1) * HEAD_DIM]
                for g in range(group)
            ],
            axis=2,
        )
        cache_scores = score_scale * jnp.einsum(
            "pbgrd,pnd->pbgrn", query, prompt_keys, preferred_element_type=jnp.float32
        )
        self_scores = score_scale * jnp.einsum(
            "pbgrd,pbud->pbgru", query, self_keys, preferred_element_type=jnp.float32
        )
        cache_mask = prompt_mask[:, None, None, None, :]
        cache_scores = jnp.where(cache_mask, cache_scores, -1e30)
        self_scores = jnp.where(self_mask, self_scores, -1e30)
        top = jnp.maximum(
            jnp.max(cache_scores, axis=-1, keepdims=True),
            jnp.max(self_scores, axis=-1, keepdims=True),
        )
        cache_weights = jnp.where(cache_mask, jnp.exp(cache_scores - top), 0.0)
        self_weights = jnp.where(self_mask, jnp.exp(self_scores - top), 0.0)
        total = jnp.sum(cache_weights, axis=-1, keepdims=True) + jnp.sum(
            self_weights, axis=-1, keepdims=True
        )
        weighted = jnp.einsum(
            "pbgrn,pnd->pbgrd",
            cache_weights.astype(jnp.bfloat16),
            prompt_values,
            preferred_element_type=jnp.float32,
        ) + jnp.einsum(
            "pbgru,pbud->pbgrd",
            self_weights.astype(jnp.bfloat16),
            self_values,
            preferred_element_type=jnp.float32,
        )
        attended = (weighted / total).astype(jnp.bfloat16)
        heads += [attended[:, :, g] for g in range(group)]
    attended = jnp.concatenate(heads, axis=-1)
    attended = attended.reshape(own_prompts, tiles, rep_count, tile * step_rows, -1)
    attended = attended.transpose(2, 0, 1, 3, 4).reshape(rep_count * row_count, -1)

    projected = (
        jnp.dot(attended, out_weight, preferred_element_type=jnp.float32)
        .astype(jnp.bfloat16)
        .reshape(rep_count, row_count, model_width)
    )
    received = [swap(projected[k], "rep", k) for k in range(1, rep_count)]
    attn_sum = projected[0].astype(jnp.float32)
    for piece in received:
        attn_sum = attn_sum + piece.astype(jnp.float32)
    attn_mixed = (own_rows.astype(jnp.float32) + attn_sum).astype(jnp.bfloat16)

    normed = normed_of(attn_mixed, moe_gain)
    chosen = jnp.take(expert_table, token_ids.reshape(row_count))
    device_count = ep_count * rep_count
    slot_total = device_count * CAP
    same_expert = chosen[:, None] == chosen[None, :]
    before = jnp.arange(row_count)[None, :] < jnp.arange(row_count)[:, None]
    slot_rank = jnp.sum((same_expert & before).astype(jnp.int32), axis=1)
    destination = chosen * CAP + slot_rank
    send_pick = (jnp.arange(slot_total, dtype=jnp.int32)[:, None] == destination[None, :]).astype(
        jnp.bfloat16
    )
    outgoing = (
        jnp.dot(send_pick, normed, preferred_element_type=jnp.float32)
        .astype(jnp.bfloat16)
        .reshape(device_count, CAP, model_width)
    )
    arrived = lax.all_to_all(outgoing, ("ep", "rep"), split_axis=0, concat_axis=0, tiled=True)
    flat_rows = arrived.reshape(slot_total, model_width)
    gate_proj = jnp.dot(flat_rows, gate_weight[0], preferred_element_type=jnp.float32)
    up_proj = jnp.dot(flat_rows, up_weight[0], preferred_element_type=jnp.float32)
    hidden = (jax.nn.silu(gate_proj) * up_proj).astype(jnp.bfloat16)
    served = (
        jnp.dot(hidden, down_weight[0], preferred_element_type=jnp.float32)
        .astype(jnp.bfloat16)
        .reshape(device_count, CAP, model_width)
    )
    returned = lax.all_to_all(served, ("ep", "rep"), split_axis=0, concat_axis=0, tiled=True)
    moe_out = lax.dot_general(
        send_pick,
        returned.reshape(slot_total, model_width),
        (((0,), (0,)), ((), ())),
        preferred_element_type=jnp.float32,
    )
    layer_out = (attn_mixed.astype(jnp.float32) + moe_out).astype(jnp.bfloat16)
    return layer_out.reshape(seqs, step_rows, model_width)


def solution(mesh):
    placed = (
        P("groups", "ep", None),
        P(("groups", "ep"), "rep", None),
        P(("groups", "ep"), None, "rep"),
        P(),
        P(None, "rep"),
        P("rep", None),
        P(),
        P(("ep", "rep"), None, None),
        P(("ep", "rep"), None, None),
        P(("ep", "rep"), None, None),
        P(),
        P("ep", "rep"),
        P("groups"),
    )
    return jax.shard_map(
        local,
        mesh=mesh,
        in_specs=placed,
        out_specs=P(("groups", "ep"), "rep", None),
        check_vma=False,
    )
```

```python
import functools
import math

import jax
import jax.numpy as jnp
from jax import lax
from jax.experimental import pallas as pl
from jax.experimental.pallas import tpu as pltpu
from jax.sharding import PartitionSpec as P

HEAD_DIM = 128
QUERY_HEADS = 16
KEY_VALUE_HEADS = 4
GROUP_PROMPTS = 4
CAP = 2

EPS = 1e-06
THETA = 1000000.0


def partner(index, step, count):
    if count & (count - 1) == 0:
        return index ^ step
    return (count + step - index) % count


def swap(block, axis, step):
    count = lax.axis_size(axis)
    return lax.ppermute(block, axis, [(i, partner(i, step, count)) for i in range(count)])


def normed_of(hidden, gain_vec):
    widened = hidden.astype(jnp.float32)
    mean_sq = jnp.mean(widened * widened, axis=-1, keepdims=True)
    return (widened * lax.rsqrt(mean_sq + EPS) * gain_vec).astype(jnp.bfloat16)


def key_value(hidden, gain_vec, key_value_weight, positions, is_key):
    rows = hidden.shape[0]
    projected = jnp.dot(
        normed_of(hidden, gain_vec), key_value_weight, preferred_element_type=jnp.float32
    )
    half = HEAD_DIM // 2
    freq = jnp.exp(jnp.arange(half, dtype=jnp.float32) * (-2.0 * math.log(THETA) / HEAD_DIM))
    angles = positions[:, None] * freq
    cosine, sine = jnp.cos(angles), jnp.sin(angles)
    out = []
    for b in range(key_value_weight.shape[1] // HEAD_DIM):
        block = projected[:, b * HEAD_DIM : (b + 1) * HEAD_DIM]
        if is_key[b] is not False:
            first, second = block[:, :half], block[:, half:]
            turned = jnp.concatenate(
                [first * cosine - second * sine, second * cosine + first * sine], axis=1
            )
            block = turned if is_key[b] is True else jnp.where(is_key[b], turned, block)
        out.append(block.astype(jnp.bfloat16))
    return jnp.concatenate(out, axis=1) if len(out) > 1 else out[0]


def general(
    prompt_hidden,
    decode_hidden,
    queries,
    attn_gain,
    key_value_weight,
    out_weight,
    moe_gain,
    gate_weight,
    up_weight,
    down_weight,
    expert_table,
    token_ids,
    prompt_lengths,
):
    seqs, step_rows, model_width = decode_hidden.shape
    prompt_len_local = prompt_hidden.shape[1]
    steps_total = queries.shape[1]
    qh_dev = queries.shape[2] // HEAD_DIM
    ep_count, rep_count = lax.axis_size("ep"), lax.axis_size("rep")
    ep_index, rep_index = lax.axis_index("ep"), lax.axis_index("rep")
    samples = seqs * ep_count // GROUP_PROMPTS
    blocks = key_value_weight.shape[1] // HEAD_DIM
    row_count = seqs * step_rows
    own_prompts = max(1, seqs // samples)

    own_rows = decode_hidden.reshape(row_count, model_width)
    others = [swap(own_rows, "rep", k) for k in range(1, rep_count)]
    owners = [partner(rep_index, k, rep_count) for k in range(rep_count)]

    if blocks == 1:
        is_key = [rep_index % 2 == 0]
    else:
        is_key = [b % 2 == 0 for b in range(blocks)]
    heads_here = max(1, blocks // 2)

    prompt_pos = (
        ep_index * prompt_len_local + jnp.arange(prompt_len_local, dtype=jnp.int32)
    ).astype(jnp.float32)
    prompt_part = key_value(
        prompt_hidden.reshape(-1, model_width),
        attn_gain,
        key_value_weight,
        jnp.tile(prompt_pos, GROUP_PROMPTS),
        is_key,
    ).reshape(GROUP_PROMPTS, prompt_len_local, blocks * HEAD_DIM)

    def first_prompt(ep):
        return ep * seqs // samples

    pieces, piece_pos = [], []
    for k in range(ep_count):
        other = partner(ep_index, k, ep_count)
        part = lax.dynamic_slice_in_dim(prompt_part, first_prompt(other), own_prompts, 0)
        pieces.append(swap(part, "ep", k) if k else part)
        piece_pos.append(other * prompt_len_local + jnp.arange(prompt_len_local, dtype=jnp.int32))
    prompt_kv = jnp.concatenate(pieces, axis=1)
    key_pos = jnp.concatenate(piece_pos)

    own_first = first_prompt(ep_index)
    own_lengths = lax.dynamic_slice_in_dim(prompt_lengths, own_first, own_prompts, 0)
    seq_lengths = jnp.repeat(own_lengths, seqs // own_prompts)

    def decode_part(k, hidden):
        step = owners[k] * step_rows + jnp.arange(step_rows, dtype=jnp.int32)
        position = (seq_lengths[:, None] + step[None, :]).astype(jnp.float32).reshape(-1)
        return position

    positions = [decode_part(k, None) for k in range(rep_count)]
    decode_own = key_value(own_rows, attn_gain, key_value_weight, positions[0], is_key)
    decode_rest = key_value(
        jnp.concatenate(others, axis=0),
        attn_gain,
        key_value_weight,
        jnp.concatenate(positions[1:]),
        is_key,
    )
    decode_kv = jnp.concatenate([decode_own, decode_rest], axis=0)
    if blocks == 1:
        partner_prompt, partner_decode = swap((prompt_kv, decode_kv), "rep", 1)
        holds_key = rep_index % 2 == 0

        def both(mine, theirs):
            return jnp.where(
                holds_key,
                jnp.concatenate([mine, theirs], axis=-1),
                jnp.concatenate([theirs, mine], axis=-1),
            )

        prompt_kv, decode_kv = both(prompt_kv, partner_prompt), both(decode_kv, partner_decode)

    tile = min(seqs // own_prompts, 8)
    tiles = seqs // own_prompts // tile
    group = qh_dev // heads_here
    by_owner = jnp.concatenate(
        [lax.dynamic_slice_in_dim(queries, o * step_rows, step_rows, 1)[None] for o in owners]
    )
    tokens = rep_count * tile * step_rows

    def tiled(rows):
        width = rows.shape[-1]
        rows = rows.reshape(rep_count, own_prompts, tiles, tile * step_rows, width)
        return rows.transpose(1, 2, 0, 3, 4).reshape(own_prompts, tiles, tokens, width)

    query_rows = tiled(by_owner.reshape(rep_count, row_count, qh_dev * HEAD_DIM))
    decode_rows = tiled(decode_kv.reshape(rep_count, row_count, -1))
    row_step = jnp.concatenate(
        [
            jnp.tile(o * step_rows + jnp.arange(step_rows, dtype=jnp.int32), tile)
            for o in owners
        ]
    )
    row_seq = jnp.tile(jnp.repeat(jnp.arange(tile, dtype=jnp.int32), step_rows), rep_count)
    self_mask = (row_seq[:, None] == row_seq[None, :]) & (row_step[None, :] <= row_step[:, None])
    prompt_mask = key_pos[None, :] < own_lengths[:, None]
    score_scale = HEAD_DIM ** (-0.5)

    heads = []
    for h in range(heads_here):
        lo = 2 * h * HEAD_DIM
        prompt_keys = prompt_kv[..., lo : lo + HEAD_DIM]
        prompt_values = prompt_kv[..., lo + HEAD_DIM : lo + 2 * HEAD_DIM]
        self_keys = decode_rows[..., lo : lo + HEAD_DIM]
        self_values = decode_rows[..., lo + HEAD_DIM : lo + 2 * HEAD_DIM]
        query = jnp.stack(
            [
                query_rows[..., (h * group + g) * HEAD_DIM : (h * group + g + 1) * HEAD_DIM]
                for g in range(group)
            ],
            axis=2,
        )
        cache_scores = score_scale * jnp.einsum(
            "pbgrd,pnd->pbgrn", query, prompt_keys, preferred_element_type=jnp.float32
        )
        self_scores = score_scale * jnp.einsum(
            "pbgrd,pbud->pbgru", query, self_keys, preferred_element_type=jnp.float32
        )
        cache_mask = prompt_mask[:, None, None, None, :]
        cache_scores = jnp.where(cache_mask, cache_scores, -1e30)
        self_scores = jnp.where(self_mask, self_scores, -1e30)
        top = jnp.maximum(
            jnp.max(cache_scores, axis=-1, keepdims=True),
            jnp.max(self_scores, axis=-1, keepdims=True),
        )
        cache_weights = jnp.where(cache_mask, jnp.exp(cache_scores - top), 0.0)
        self_weights = jnp.where(self_mask, jnp.exp(self_scores - top), 0.0)
        total = jnp.sum(cache_weights, axis=-1, keepdims=True) + jnp.sum(
            self_weights, axis=-1, keepdims=True
        )
        weighted = jnp.einsum(
            "pbgrn,pnd->pbgrd",
            cache_weights.astype(jnp.bfloat16),
            prompt_values,
            preferred_element_type=jnp.float32,
        ) + jnp.einsum(
            "pbgru,pbud->pbgrd",
            self_weights.astype(jnp.bfloat16),
            self_values,
            preferred_element_type=jnp.float32,
        )
        attended = (weighted / total).astype(jnp.bfloat16)
        heads += [attended[:, :, g] for g in range(group)]
    attended = jnp.concatenate(heads, axis=-1)
    attended = attended.reshape(own_prompts, tiles, rep_count, tile * step_rows, -1)
    attended = attended.transpose(2, 0, 1, 3, 4).reshape(rep_count * row_count, -1)

    projected = (
        jnp.dot(attended, out_weight, preferred_element_type=jnp.float32)
        .astype(jnp.bfloat16)
        .reshape(rep_count, row_count, model_width)
    )
    received = [swap(projected[k], "rep", k) for k in range(1, rep_count)]
    attn_sum = projected[0].astype(jnp.float32)
    for piece in received:
        attn_sum = attn_sum + piece.astype(jnp.float32)
    attn_mixed = (own_rows.astype(jnp.float32) + attn_sum).astype(jnp.bfloat16)

    normed = normed_of(attn_mixed, moe_gain)
    chosen = jnp.take(expert_table, token_ids.reshape(row_count))
    device_count = ep_count * rep_count
    slot_total = device_count * CAP
    same_expert = chosen[:, None] == chosen[None, :]
    before = jnp.arange(row_count)[None, :] < jnp.arange(row_count)[:, None]
    slot_rank = jnp.sum((same_expert & before).astype(jnp.int32), axis=1)
    destination = chosen * CAP + slot_rank
    send_pick = (jnp.arange(slot_total, dtype=jnp.int32)[:, None] == destination[None, :]).astype(
        jnp.bfloat16
    )
    outgoing = (
        jnp.dot(send_pick, normed, preferred_element_type=jnp.float32)
        .astype(jnp.bfloat16)
        .reshape(device_count, CAP, model_width)
    )
    arrived = lax.all_to_all(outgoing, ("ep", "rep"), split_axis=0, concat_axis=0, tiled=True)
    flat_rows = arrived.reshape(slot_total, model_width)
    gate_proj = jnp.dot(flat_rows, gate_weight[0], preferred_element_type=jnp.float32)
    up_proj = jnp.dot(flat_rows, up_weight[0], preferred_element_type=jnp.float32)
    hidden = (jax.nn.silu(gate_proj) * up_proj).astype(jnp.bfloat16)
    served = (
        jnp.dot(hidden, down_weight[0], preferred_element_type=jnp.float32)
        .astype(jnp.bfloat16)
        .reshape(device_count, CAP, model_width)
    )
    returned = lax.all_to_all(served, ("ep", "rep"), split_axis=0, concat_axis=0, tiled=True)
    moe_out = lax.dot_general(
        send_pick,
        returned.reshape(slot_total, model_width),
        (((0,), (0,)), ((), ())),
        preferred_element_type=jnp.float32,
    )
    layer_out = (attn_mixed.astype(jnp.float32) + moe_out).astype(jnp.bfloat16)
    return layer_out.reshape(seqs, step_rows, model_width)


GRANT = 16 << 20
VMEM = pl.BlockSpec(memory_space=pltpu.VMEM)


def on_chip(shape, dtype):
    return pltpu.VMEM(shape, dtype)


def far(*arrays):
    return [pltpu.with_memory_space_constraint(a, pltpu.HBM) for a in arrays]


def held(*arrays):
    return [pltpu.with_memory_space_constraint(a, pltpu.VMEM) for a in arrays]


def angles_of(positions):
    half = HEAD_DIM // 2
    lane = lax.broadcasted_iota(jnp.int32, (1, HEAD_DIM), 1)
    spot = jnp.where(lane < half, lane, lane - half).astype(jnp.float32)
    angles = positions * jnp.exp(spot * (-2.0 * math.log(THETA) / HEAD_DIM))
    sine = jnp.sin(angles)
    return jnp.cos(angles), jnp.where(lane < half, -sine, sine)


def turn(block, cosine, sine):
    return block * cosine + pltpu.roll(block, HEAD_DIM // 2, 1) * sine


def column(count):
    return lax.broadcasted_iota(jnp.int32, (count, 1), 0)


HBM = pl.BlockSpec(memory_space=pltpu.HBM)


def fetch(pairs, sems):
    copies = [pltpu.make_async_copy(a, b, sems.at[i]) for i, (a, b) in enumerate(pairs)]
    for copy in copies:
        copy.start()
    return copies


def prompt_kernel(seqs, samples, hidden, gain, weight, decode, queries, *rest):
    *outs, gain_out, weight_out, decode_out, queries_out, rows, scratch, sems = rest
    copies = fetch(
        [
            (hidden, rows),
            (gain, gain_out),
            (weight, weight_out),
            (decode, decode_out),
            (queries, queries_out),
        ],
        sems,
    )
    prompts, here, width = hidden.shape
    ep = lax.axis_index("ep")
    spot = lax.rem(column(prompts * here), here) + ep * here
    cosine, sine = angles_of(spot.astype(jnp.float32))
    copies[0].wait()
    copies[1].wait()
    normed = normed_of(rows[...].astype(jnp.float32).reshape(prompts * here, width), gain_out[...])
    copies[2].wait()
    projected = jnp.dot(normed, weight_out[...], preferred_element_type=jnp.float32)
    keys = turn(projected[:, :HEAD_DIM], cosine, sine)
    scratch[:, :, :HEAD_DIM] = keys.reshape(prompts, here, HEAD_DIM)
    scratch[:, :, HEAD_DIM:] = projected[:, HEAD_DIM:].reshape(prompts, here, HEAD_DIM)
    for k, out in enumerate(outs):
        first = partner(ep, k, len(outs)) * seqs // samples
        out[...] = scratch[first].astype(jnp.bfloat16)
    copies[3].wait()
    copies[4].wait()


def prompt_part(prompt_hidden, gain, weight, decode_hidden, queries, samples, ep_count):
    prompts, here, _ = prompt_hidden.shape
    columns = weight.shape[1]
    copied = [gain, weight, decode_hidden, queries]
    return pl.pallas_call(
        functools.partial(prompt_kernel, decode_hidden.shape[0], samples),
        out_shape=[on_chip((here, columns), jnp.bfloat16)] * ep_count
        + [on_chip(a.shape, a.dtype) for a in copied],
        in_specs=[HBM] * 5,
        out_specs=[VMEM] * (ep_count + 4),
        scratch_shapes=[
            pltpu.VMEM(prompt_hidden.shape, prompt_hidden.dtype),
            pltpu.VMEM((prompts, here, columns), jnp.float32),
            pltpu.SemaphoreType.DMA((5,)),
        ],
        compiler_params=pltpu.CompilerParams(vmem_limit_bytes=GRANT),
        name="prompt_part",
    )(*far(prompt_hidden, gain, weight, decode_hidden, queries))


def place(rep, reps, own, step_rows, index):
    k = index // own
    sequence = lax.rem(index, own) // step_rows
    return partner(rep, k, reps) * step_rows + lax.rem(index, step_rows), sequence


def decode_kernel(reps, eps, here, samples, lengths, out_weight, gain, weight, queries, *rest):
    hidden, (key_value, ordered, mask, own_rows, out_copy, rows, sizes, sems) = rest[:reps], rest[reps:]
    copies = fetch([(lengths, sizes), (out_weight, out_copy)], sems)
    seqs, steps, _ = queries.shape
    step_rows = steps // reps
    own = seqs * step_rows
    total = reps * own
    ep, rep = lax.axis_index("ep"), lax.axis_index("rep")
    for k, piece in enumerate(hidden):
        for s in range(seqs):
            at = k * own + s * step_rows
            rows[at : at + step_rows, :] = piece[s]
    copies[0].wait()
    length = sizes[ep * seqs // samples]
    row_step, row_seq = place(rep, reps, own, step_rows, column(total))
    cosine, sine = angles_of((row_step + length).astype(jnp.float32))
    normed = normed_of(rows[...], gain[...])
    projected = jnp.dot(normed, weight[...], preferred_element_type=jnp.float32)
    key_value[:, :HEAD_DIM] = turn(projected[:, :HEAD_DIM], cosine, sine).astype(jnp.bfloat16)
    key_value[:, HEAD_DIM:] = projected[:, HEAD_DIM:].astype(jnp.bfloat16)
    source = row_seq * steps + row_step
    pick = (source == lax.broadcasted_iota(jnp.int32, (total, total), 1)).astype(jnp.bfloat16)
    flat = queries[...].astype(jnp.float32).reshape(total, -1).astype(jnp.bfloat16)
    query = jnp.dot(pick, flat, preferred_element_type=jnp.float32).astype(jnp.bfloat16)
    for g in range(query.shape[1] // HEAD_DIM):
        ordered[g * total : (g + 1) * total, :] = query[:, g * HEAD_DIM : (g + 1) * HEAD_DIM]
    own_rows[...] = rows[:own, :]
    key = lax.broadcasted_iota(jnp.int32, (1, eps * here + total), 1)
    key_ep = partner(ep, key // here, eps)
    prompt_ok = (key < eps * here) & (key_ep * here + lax.rem(key, here) < length)
    key_step, key_seq = place(rep, reps, own, step_rows, key - eps * here)
    self_ok = (key >= eps * here) & (key_seq == row_seq) & (key_step <= row_step)
    mask[...] = (prompt_ok | self_ok).astype(jnp.int32)
    copies[1].wait()


def decode_part(lengths, out_weight, gain, weight, queries, hidden, here, eps, samples):
    seqs, steps, columns = queries.shape
    total, width = seqs * steps, out_weight.shape[1]
    return pl.pallas_call(
        functools.partial(decode_kernel, len(hidden), eps, here, samples),
        out_shape=[
            on_chip((total, weight.shape[1]), jnp.bfloat16),
            on_chip((total * columns // HEAD_DIM, HEAD_DIM), jnp.bfloat16),
            on_chip((total, eps * here + total), jnp.int32),
            on_chip((total // len(hidden), width), jnp.bfloat16),
            on_chip(out_weight.shape, out_weight.dtype),
        ],
        in_specs=[HBM] * 2 + [VMEM] * (3 + len(hidden)),
        out_specs=[VMEM] * 5,
        scratch_shapes=[
            pltpu.VMEM((total, width), jnp.bfloat16),
            pltpu.SMEM(lengths.shape, jnp.int32),
            pltpu.SemaphoreType.DMA((2,)),
        ],
        compiler_params=pltpu.CompilerParams(vmem_limit_bytes=GRANT),
        name="decode_part",
    )(*far(lengths, out_weight), gain, weight, queries, *hidden)


def attend_kernel(key_value, query, mask, own_rows, out_weight, *rest):
    own, total = own_rows.shape[0], key_value.shape[0]
    reps = total // own
    prompts, outs = rest[:-reps], rest[-reps:]
    group = query.shape[0] // total
    keys = jnp.concatenate([p[:, :HEAD_DIM] for p in prompts] + [key_value[:, :HEAD_DIM]], axis=0)
    values = jnp.concatenate([p[:, HEAD_DIM:] for p in prompts] + [key_value[:, HEAD_DIM:]], axis=0)
    scores = lax.dot_general(
        query[...], keys, (((1,), (1,)), ((), ())), preferred_element_type=jnp.float32
    ) * (HEAD_DIM**-0.5)
    admitted = jnp.concatenate([mask[...]] * group, axis=0) != 0
    scores = jnp.where(admitted, scores, -1e30)
    top = jnp.max(scores, axis=1, keepdims=True)
    weights = jnp.where(admitted, jnp.exp(scores - top), 0.0)
    row_total = jnp.sum(weights, axis=1, keepdims=True)
    weighted = jnp.dot(weights.astype(jnp.bfloat16), values, preferred_element_type=jnp.float32)
    attended = (weighted / row_total).astype(jnp.bfloat16)
    attended = jnp.concatenate(
        [attended[g * total : (g + 1) * total] for g in range(group)], axis=1
    )
    projected = jnp.dot(attended, out_weight[...], preferred_element_type=jnp.float32)
    for k in range(reps):
        part = projected[k * own : (k + 1) * own]
        if k == 0:
            part = part + own_rows[...].astype(jnp.float32)
        outs[k][...] = part.astype(outs[k].dtype)


def attend_part(key_value, query, mask, own_rows, out_weight, prompts):
    own, width = own_rows.shape
    reps = key_value.shape[0] // own
    shapes = [on_chip((own, width), jnp.float32)]
    shapes += [on_chip((own, width), jnp.bfloat16)] * (reps - 1)
    return pl.pallas_call(
        attend_kernel,
        out_shape=shapes,
        in_specs=[VMEM] * (5 + len(prompts)),
        out_specs=[VMEM] * reps,
        compiler_params=pltpu.CompilerParams(vmem_limit_bytes=GRANT),
        name="attend_part",
    )(key_value, query, mask, own_rows, out_weight, *prompts)


def route_kernel(after, ids, table, gain, gate, up, down, pick, pick_back, *rest):
    del after
    gain_out, gate_out, up_out, down_out, token_ids, lines, sems = rest
    copies = fetch(
        [
            (ids, token_ids),
            (table, lines),
            (gain, gain_out),
            (gate, gate_out),
            (up, up_out),
            (down, down_out),
        ],
        sems,
    )
    step_rows, seqs = token_ids.shape
    count, lanes = seqs * step_rows, table.shape[1]
    lane = lax.broadcasted_iota(jnp.int32, (1, lanes), 1)
    across = jnp.full((1, count), -1, jnp.int32)
    below = jnp.full((count, 1), -1, jnp.int32)
    spot = lax.broadcasted_iota(jnp.int32, (1, count), 1)
    copies[0].wait()
    copies[1].wait()
    for i in range(count):
        token = token_ids[i % step_rows, i // step_rows]
        line = lines[pl.ds(token // lanes, 1), :]
        found = jnp.sum(jnp.where(lane == lax.rem(token, lanes), line, 0), axis=1, keepdims=True)
        across = jnp.where(spot == i, found, across)
        below = jnp.where(column(count) == i, found, below)
    same = across == below
    rank = jnp.sum((same & (column(count) < spot)).astype(jnp.int32), axis=0, keepdims=True)
    rank_below = jnp.sum((same & (spot < column(count))).astype(jnp.int32), axis=1, keepdims=True)
    slots = pick.shape[0]
    pick[...] = (column(slots) == across * CAP + rank).astype(jnp.bfloat16)
    slot = lax.broadcasted_iota(jnp.int32, (1, slots), 1)
    pick_back[...] = (slot == below * CAP + rank_below).astype(jnp.bfloat16)
    for copy in copies[2:]:
        copy.wait()


def route_part(after, token_ids, table, weights, slots):
    count = token_ids.size
    token_ids, table = token_ids.T, table.reshape(-1, 128)
    return pl.pallas_call(
        route_kernel,
        out_shape=[
            on_chip((slots, count), jnp.bfloat16),
            on_chip((count, slots), jnp.bfloat16),
        ]
        + [on_chip(w.shape, w.dtype) for w in weights],
        in_specs=[VMEM] + [HBM] * (2 + len(weights)),
        out_specs=[VMEM] * (2 + len(weights)),
        scratch_shapes=[
            pltpu.SMEM(token_ids.shape, jnp.int32),
            pltpu.VMEM(table.shape, table.dtype),
            pltpu.SemaphoreType.DMA((2 + len(weights),)),
        ],
        compiler_params=pltpu.CompilerParams(vmem_limit_bytes=GRANT),
        name="route_part",
    )(after, *far(token_ids, table, *weights))


def send_kernel(gain, pick, own, *rest):
    *others, mixed, outgoing = rest
    total = own[...]
    for piece in others:
        total = total + piece[...].astype(jnp.float32)
    rounded = total.astype(jnp.bfloat16)
    mixed[...] = rounded
    normed = normed_of(rounded, gain[...])
    slots = jnp.dot(pick[...], normed, preferred_element_type=jnp.float32).astype(jnp.bfloat16)
    for d in range(outgoing.shape[0]):
        outgoing[d] = slots[d * CAP : (d + 1) * CAP]


def send_part(gain, pick, shares):
    rows, width = shares[0].shape
    return pl.pallas_call(
        send_kernel,
        out_shape=[
            on_chip((rows, width), jnp.bfloat16),
            on_chip((pick.shape[0] // CAP, CAP, width), jnp.bfloat16),
        ],
        in_specs=[VMEM] * (2 + len(shares)),
        out_specs=[VMEM] * 2,
        compiler_params=pltpu.CompilerParams(vmem_limit_bytes=GRANT),
        name="send_part",
    )(gain, pick, *shares)


def expert_kernel(arrived, gate_weight, up_weight, down_weight, served, rows):
    for d in range(arrived.shape[0]):
        rows[d * CAP : (d + 1) * CAP, :] = arrived[d]
    tokens = rows[...]
    gate_proj = jnp.dot(tokens, gate_weight[0], preferred_element_type=jnp.float32)
    up_proj = jnp.dot(tokens, up_weight[0], preferred_element_type=jnp.float32)
    hidden = (gate_proj / (1.0 + jnp.exp(-gate_proj)) * up_proj).astype(jnp.bfloat16)
    result = jnp.dot(hidden, down_weight[0], preferred_element_type=jnp.float32)
    result = result.astype(jnp.bfloat16)
    for d in range(served.shape[0]):
        served[d] = result[d * CAP : (d + 1) * CAP]


def expert_part(arrived, gate_weight, up_weight, down_weight):
    return pl.pallas_call(
        expert_kernel,
        out_shape=on_chip(arrived.shape, jnp.bfloat16),
        in_specs=[VMEM] * 4,
        out_specs=VMEM,
        scratch_shapes=[pltpu.VMEM((arrived.shape[0] * CAP, arrived.shape[2]), jnp.bfloat16)],
        compiler_params=pltpu.CompilerParams(vmem_limit_bytes=GRANT),
        name="expert_part",
    )(arrived, gate_weight, up_weight, down_weight)


def final_kernel(pick_back, mixed, returned, out, rows):
    for d in range(returned.shape[0]):
        rows[d * CAP : (d + 1) * CAP, :] = returned[d]
    moe_out = jnp.dot(pick_back[...], rows[...], preferred_element_type=jnp.float32)
    total = (mixed[...].astype(jnp.float32) + moe_out).astype(jnp.bfloat16)
    step_rows = out.shape[1]
    for s in range(out.shape[0]):
        out[s] = total[s * step_rows : (s + 1) * step_rows]


def final_part(pick_back, mixed, returned, shape):
    return pl.pallas_call(
        final_kernel,
        out_shape=jax.ShapeDtypeStruct(shape, jnp.bfloat16),
        in_specs=[VMEM] * 3,
        out_specs=VMEM,
        scratch_shapes=[pltpu.VMEM((returned.shape[0] * CAP, returned.shape[2]), jnp.bfloat16)],
        compiler_params=pltpu.CompilerParams(vmem_limit_bytes=GRANT),
        name="final_part",
    )(pick_back, mixed, returned)


def local(
    prompt_hidden,
    decode_hidden,
    queries,
    attn_gain,
    key_value_weight,
    out_weight,
    moe_gain,
    gate_weight,
    up_weight,
    down_weight,
    expert_table,
    token_ids,
    prompt_lengths,
):
    seqs = decode_hidden.shape[0]
    ep_count, rep_count = lax.axis_size("ep"), lax.axis_size("rep")
    samples = seqs * ep_count // GROUP_PROMPTS
    blocks = key_value_weight.shape[1] // HEAD_DIM
    if blocks != 2 or seqs > 8 or samples % seqs or expert_table.shape[0] % 128:
        return general(
            prompt_hidden,
            decode_hidden,
            queries,
            attn_gain,
            key_value_weight,
            out_weight,
            moe_gain,
            gate_weight,
            up_weight,
            down_weight,
            expert_table,
            token_ids,
            prompt_lengths,
        )
    attn_gain, moe_gain = attn_gain[None, :], moe_gain[None, :]
    others = [swap(decode_hidden, "rep", k) for k in range(1, rep_count)]
    *parts, gain, weight, own_hidden, query = prompt_part(
        prompt_hidden, attn_gain, key_value_weight, decode_hidden, queries, samples, ep_count
    )
    prompts = [swap(part, "ep", k) if k else part for k, part in enumerate(parts)]
    *ready, out_weight = decode_part(
        prompt_lengths,
        out_weight,
        *held(gain, weight, query),
        held(own_hidden, *others),
        prompt_hidden.shape[1],
        ep_count,
        samples,
    )
    shares = attend_part(*held(*ready, out_weight), held(*prompts))
    pick, pick_back, moe_gain, *weights = route_part(
        shares[0],
        token_ids,
        expert_table,
        (moe_gain, gate_weight, up_weight, down_weight),
        ep_count * rep_count * CAP,
    )
    shares = [swap(share, "rep", k) if k else share for k, share in enumerate(shares)]
    mixed, outgoing = send_part(moe_gain, pick, held(*shares))
    arrived = lax.all_to_all(outgoing, ("ep", "rep"), split_axis=0, concat_axis=0, tiled=True)
    served = expert_part(*held(arrived, *weights))
    returned = lax.all_to_all(served, ("ep", "rep"), split_axis=0, concat_axis=0, tiled=True)
    return final_part(pick_back, mixed, *held(returned), decode_hidden.shape)


def solution(mesh):
    placed = (
        P("groups", "ep", None),
        P(("groups", "ep"), "rep", None),
        P(("groups", "ep"), None, "rep"),
        P(),
        P(None, "rep"),
        P("rep", None),
        P(),
        P(("ep", "rep"), None, None),
        P(("ep", "rep"), None, None),
        P(("ep", "rep"), None, None),
        P(),
        P("ep", "rep"),
        P("groups"),
    )
    return jax.shard_map(
        local,
        mesh=mesh,
        in_specs=placed,
        out_specs=P(("groups", "ep"), "rep", None),
        check_vma=False,
    )
```

```python
import functools
import math

import jax
import jax.numpy as jnp
from jax import lax
from jax.experimental import pallas as pl
from jax.experimental.pallas import tpu as pltpu
from jax.sharding import PartitionSpec as P


HEAD_DIM = 128
GROUP_PROMPTS = 4
CAP = 2

EPS = 1e-06
THETA = 1000000.0


def partner(index, step, count):
    if count & (count - 1) == 0:
        return index ^ step
    return (count + step - index) % count


def swap(block, axis, step):
    count = lax.axis_size(axis)
    return lax.ppermute(block, axis, [(i, partner(i, step, count)) for i in range(count)])


def normed_of(hidden, gain_vec):
    widened = hidden.astype(jnp.float32)
    mean_sq = jnp.mean(widened * widened, axis=-1, keepdims=True)
    return (widened * lax.rsqrt(mean_sq + EPS) * gain_vec).astype(jnp.bfloat16)


def key_value(hidden, gain_vec, key_value_weight, positions, is_key):
    projected = jnp.dot(
        normed_of(hidden, gain_vec), key_value_weight, preferred_element_type=jnp.float32
    )
    half = HEAD_DIM // 2
    freq = jnp.exp(jnp.arange(half, dtype=jnp.float32) * (-2.0 * math.log(THETA) / HEAD_DIM))
    angles = positions[:, None] * freq
    cosine, sine = jnp.cos(angles), jnp.sin(angles)
    out = []
    for b in range(key_value_weight.shape[1] // HEAD_DIM):
        block = projected[:, b * HEAD_DIM : (b + 1) * HEAD_DIM]
        if is_key[b] is not False:
            first, second = block[:, :half], block[:, half:]
            turned = jnp.concatenate(
                [first * cosine - second * sine, second * cosine + first * sine], axis=1
            )
            block = turned if is_key[b] is True else jnp.where(is_key[b], turned, block)
        out.append(block.astype(jnp.bfloat16))
    return jnp.concatenate(out, axis=1) if len(out) > 1 else out[0]


def general(
    prompt_hidden,
    decode_hidden,
    queries,
    attn_gain,
    key_value_weight,
    out_weight,
    moe_gain,
    gate_weight,
    up_weight,
    down_weight,
    expert_table,
    token_ids,
    prompt_lengths,
):
    seqs, step_rows, model_width = decode_hidden.shape
    prompt_len_local = prompt_hidden.shape[1]
    qh_dev = queries.shape[2] // HEAD_DIM
    ep_count, rep_count = lax.axis_size("ep"), lax.axis_size("rep")
    ep_index, rep_index = lax.axis_index("ep"), lax.axis_index("rep")
    samples = seqs * ep_count // GROUP_PROMPTS
    blocks = key_value_weight.shape[1] // HEAD_DIM
    row_count = seqs * step_rows
    own_prompts = max(1, seqs // samples)

    own_rows = decode_hidden.reshape(row_count, model_width)
    others = [swap(own_rows, "rep", k) for k in range(1, rep_count)]
    owners = [partner(rep_index, k, rep_count) for k in range(rep_count)]

    if blocks == 1:
        is_key = [rep_index % 2 == 0]
    else:
        is_key = [b % 2 == 0 for b in range(blocks)]
    heads_here = max(1, blocks // 2)

    prompt_pos = (
        ep_index * prompt_len_local + jnp.arange(prompt_len_local, dtype=jnp.int32)
    ).astype(jnp.float32)
    prompt_part = key_value(
        prompt_hidden.reshape(-1, model_width),
        attn_gain,
        key_value_weight,
        jnp.tile(prompt_pos, GROUP_PROMPTS),
        is_key,
    ).reshape(GROUP_PROMPTS, prompt_len_local, blocks * HEAD_DIM)

    def first_prompt(ep):
        return ep * seqs // samples

    pieces, piece_pos = [], []
    for k in range(ep_count):
        other = partner(ep_index, k, ep_count)
        part = lax.dynamic_slice_in_dim(prompt_part, first_prompt(other), own_prompts, 0)
        pieces.append(swap(part, "ep", k) if k else part)
        piece_pos.append(other * prompt_len_local + jnp.arange(prompt_len_local, dtype=jnp.int32))
    prompt_kv = jnp.concatenate(pieces, axis=1)
    key_pos = jnp.concatenate(piece_pos)

    own_first = first_prompt(ep_index)
    own_lengths = lax.dynamic_slice_in_dim(prompt_lengths, own_first, own_prompts, 0)
    seq_lengths = jnp.repeat(own_lengths, seqs // own_prompts)

    def decode_part(k):
        step = owners[k] * step_rows + jnp.arange(step_rows, dtype=jnp.int32)
        position = (seq_lengths[:, None] + step[None, :]).astype(jnp.float32).reshape(-1)
        return position

    positions = [decode_part(k) for k in range(rep_count)]
    decode_own = key_value(own_rows, attn_gain, key_value_weight, positions[0], is_key)
    decode_rest = key_value(
        jnp.concatenate(others, axis=0),
        attn_gain,
        key_value_weight,
        jnp.concatenate(positions[1:]),
        is_key,
    )
    decode_kv = jnp.concatenate([decode_own, decode_rest], axis=0)
    if blocks == 1:
        partner_prompt, partner_decode = swap((prompt_kv, decode_kv), "rep", 1)
        holds_key = rep_index % 2 == 0

        def both(mine, theirs):
            return jnp.where(
                holds_key,
                jnp.concatenate([mine, theirs], axis=-1),
                jnp.concatenate([theirs, mine], axis=-1),
            )

        prompt_kv, decode_kv = both(prompt_kv, partner_prompt), both(decode_kv, partner_decode)

    tile = min(seqs // own_prompts, 8)
    tiles = seqs // own_prompts // tile
    group = qh_dev // heads_here
    by_owner = jnp.concatenate(
        [lax.dynamic_slice_in_dim(queries, o * step_rows, step_rows, 1)[None] for o in owners]
    )
    tokens = rep_count * tile * step_rows

    def tiled(rows):
        width = rows.shape[-1]
        rows = rows.reshape(rep_count, own_prompts, tiles, tile * step_rows, width)
        return rows.transpose(1, 2, 0, 3, 4).reshape(own_prompts, tiles, tokens, width)

    query_rows = tiled(by_owner.reshape(rep_count, row_count, qh_dev * HEAD_DIM))
    decode_rows = tiled(decode_kv.reshape(rep_count, row_count, -1))
    row_step = jnp.concatenate(
        [
            jnp.tile(o * step_rows + jnp.arange(step_rows, dtype=jnp.int32), tile)
            for o in owners
        ]
    )
    row_seq = jnp.tile(jnp.repeat(jnp.arange(tile, dtype=jnp.int32), step_rows), rep_count)
    self_mask = (row_seq[:, None] == row_seq[None, :]) & (row_step[None, :] <= row_step[:, None])
    prompt_mask = key_pos[None, :] < own_lengths[:, None]
    score_scale = HEAD_DIM ** (-0.5)

    heads = []
    for h in range(heads_here):
        lo = 2 * h * HEAD_DIM
        prompt_keys = prompt_kv[..., lo : lo + HEAD_DIM]
        prompt_values = prompt_kv[..., lo + HEAD_DIM : lo + 2 * HEAD_DIM]
        self_keys = decode_rows[..., lo : lo + HEAD_DIM]
        self_values = decode_rows[..., lo + HEAD_DIM : lo + 2 * HEAD_DIM]
        query = jnp.stack(
            [
                query_rows[..., (h * group + g) * HEAD_DIM : (h * group + g + 1) * HEAD_DIM]
                for g in range(group)
            ],
            axis=2,
        )
        cache_scores = score_scale * jnp.einsum(
            "pbgrd,pnd->pbgrn", query, prompt_keys, preferred_element_type=jnp.float32
        )
        self_scores = score_scale * jnp.einsum(
            "pbgrd,pbud->pbgru", query, self_keys, preferred_element_type=jnp.float32
        )
        cache_mask = prompt_mask[:, None, None, None, :]
        cache_scores = jnp.where(cache_mask, cache_scores, -1e30)
        self_scores = jnp.where(self_mask, self_scores, -1e30)
        top = jnp.maximum(
            jnp.max(cache_scores, axis=-1, keepdims=True),
            jnp.max(self_scores, axis=-1, keepdims=True),
        )
        cache_weights = jnp.where(cache_mask, jnp.exp(cache_scores - top), 0.0)
        self_weights = jnp.where(self_mask, jnp.exp(self_scores - top), 0.0)
        total = jnp.sum(cache_weights, axis=-1, keepdims=True) + jnp.sum(
            self_weights, axis=-1, keepdims=True
        )
        weighted = jnp.einsum(
            "pbgrn,pnd->pbgrd",
            cache_weights.astype(jnp.bfloat16),
            prompt_values,
            preferred_element_type=jnp.float32,
        ) + jnp.einsum(
            "pbgru,pbud->pbgrd",
            self_weights.astype(jnp.bfloat16),
            self_values,
            preferred_element_type=jnp.float32,
        )
        attended = (weighted / total).astype(jnp.bfloat16)
        heads += [attended[:, :, g] for g in range(group)]
    attended = jnp.concatenate(heads, axis=-1)
    attended = attended.reshape(own_prompts, tiles, rep_count, tile * step_rows, -1)
    attended = attended.transpose(2, 0, 1, 3, 4).reshape(rep_count * row_count, -1)

    projected = (
        jnp.dot(attended, out_weight, preferred_element_type=jnp.float32)
        .astype(jnp.bfloat16)
        .reshape(rep_count, row_count, model_width)
    )
    received = [swap(projected[k], "rep", k) for k in range(1, rep_count)]
    attn_sum = projected[0].astype(jnp.float32)
    for piece in received:
        attn_sum = attn_sum + piece.astype(jnp.float32)
    attn_mixed = (own_rows.astype(jnp.float32) + attn_sum).astype(jnp.bfloat16)

    normed = normed_of(attn_mixed, moe_gain)
    chosen = jnp.take(expert_table, token_ids.reshape(row_count))
    device_count = ep_count * rep_count
    slot_total = device_count * CAP
    same_expert = chosen[:, None] == chosen[None, :]
    before = jnp.arange(row_count)[None, :] < jnp.arange(row_count)[:, None]
    slot_rank = jnp.sum((same_expert & before).astype(jnp.int32), axis=1)
    destination = chosen * CAP + slot_rank
    send_pick = (jnp.arange(slot_total, dtype=jnp.int32)[:, None] == destination[None, :]).astype(
        jnp.bfloat16
    )
    outgoing = (
        jnp.dot(send_pick, normed, preferred_element_type=jnp.float32)
        .astype(jnp.bfloat16)
        .reshape(device_count, CAP, model_width)
    )
    arrived = lax.all_to_all(outgoing, ("ep", "rep"), split_axis=0, concat_axis=0, tiled=True)
    flat_rows = arrived.reshape(slot_total, model_width)
    gate_proj = jnp.dot(flat_rows, gate_weight[0], preferred_element_type=jnp.float32)
    up_proj = jnp.dot(flat_rows, up_weight[0], preferred_element_type=jnp.float32)
    hidden = (jax.nn.silu(gate_proj) * up_proj).astype(jnp.bfloat16)
    served = (
        jnp.dot(hidden, down_weight[0], preferred_element_type=jnp.float32)
        .astype(jnp.bfloat16)
        .reshape(device_count, CAP, model_width)
    )
    returned = lax.all_to_all(served, ("ep", "rep"), split_axis=0, concat_axis=0, tiled=True)
    moe_out = lax.dot_general(
        send_pick,
        returned.reshape(slot_total, model_width),
        (((0,), (0,)), ((), ())),
        preferred_element_type=jnp.float32,
    )
    layer_out = (attn_mixed.astype(jnp.float32) + moe_out).astype(jnp.bfloat16)
    return layer_out.reshape(seqs, step_rows, model_width)


GRANT = 16 << 20
SPAN = pl.CostEstimate(flops=1 << 32, transcendentals=0, bytes_accessed=1 << 20)
VMEM = pl.BlockSpec(memory_space=pltpu.VMEM)


def on_chip(shape, dtype):
    return pltpu.VMEM(shape, dtype)


def far(*arrays):
    return [pltpu.with_memory_space_constraint(a, pltpu.HBM) for a in arrays]


def held(*arrays):
    return [pltpu.with_memory_space_constraint(a, pltpu.VMEM) for a in arrays]


def angles_of(positions):
    half = HEAD_DIM // 2
    lane = lax.broadcasted_iota(jnp.int32, (1, HEAD_DIM), 1)
    spot = jnp.where(lane < half, lane, lane - half).astype(jnp.float32)
    angles = positions * jnp.exp(spot * (-2.0 * math.log(THETA) / HEAD_DIM))
    sine = jnp.sin(angles)
    return jnp.cos(angles), jnp.where(lane < half, -sine, sine)


def turn(block, cosine, sine):
    return block * cosine + pltpu.roll(block, HEAD_DIM // 2, 1) * sine


def column(count):
    return lax.broadcasted_iota(jnp.int32, (count, 1), 0)


HBM = pl.BlockSpec(memory_space=pltpu.HBM)


def ahead_kernel(out):
    out[...] = jnp.zeros(out.shape, out.dtype)


def ahead_part():
    return pl.pallas_call(
        ahead_kernel,
        out_shape=on_chip((8, HEAD_DIM), jnp.float32),
        out_specs=VMEM,
        compiler_params=pltpu.CompilerParams(vmem_limit_bytes=GRANT),
        cost_estimate=SPAN,
        name="ahead_part",
    )()


def prompt_kernel(seqs, samples, ahead, hidden, gain, weight, *rest):
    del ahead
    *outs, scratch = rest
    prompts, here, width = hidden.shape
    ep = lax.axis_index("ep")
    spot = lax.rem(column(prompts * here), here) + ep * here
    cosine, sine = angles_of(spot.astype(jnp.float32))
    normed = normed_of(hidden[...].astype(jnp.float32).reshape(prompts * here, width), gain[...])
    projected = jnp.dot(normed, weight[...], preferred_element_type=jnp.float32)
    keys = turn(projected[:, :HEAD_DIM], cosine, sine)
    scratch[:, :, :HEAD_DIM] = keys.reshape(prompts, here, HEAD_DIM)
    scratch[:, :, HEAD_DIM:] = projected[:, HEAD_DIM:].reshape(prompts, here, HEAD_DIM)
    for k, out in enumerate(outs):
        first = partner(ep, k, len(outs)) * seqs // samples
        out[...] = scratch[first].astype(jnp.bfloat16)


def prompt_part(ahead, prompt_hidden, gain, weight, seqs, samples, ep_count):
    prompts, here, _ = prompt_hidden.shape
    columns = weight.shape[1]
    return pl.pallas_call(
        functools.partial(prompt_kernel, seqs, samples),
        out_shape=[on_chip((here, columns), jnp.bfloat16)] * ep_count,
        in_specs=[VMEM] * 4,
        out_specs=[VMEM] * ep_count,
        scratch_shapes=[pltpu.VMEM((prompts, here, columns), jnp.float32)],
        compiler_params=pltpu.CompilerParams(vmem_limit_bytes=GRANT),
        cost_estimate=SPAN,
        name="prompt_part",
    )(ahead, prompt_hidden, gain, weight)


def place(rep, reps, own, step_rows, index):
    k = index // own
    sequence = lax.rem(index, own) // step_rows
    return partner(rep, k, reps) * step_rows + lax.rem(index, step_rows), sequence


def ready_kernel(reps, eps, here, samples, lengths, gain, weight, decode, queries, *rest):
    ordered, mask, cosine_out, sine_out, own_kv, own_rows = rest
    seqs, steps, _ = queries.shape
    step_rows = steps // reps
    own = seqs * step_rows
    total = reps * own
    ep, rep = lax.axis_index("ep"), lax.axis_index("rep")
    row_step, row_seq = place(rep, reps, own, step_rows, column(total))
    source = row_seq * steps + row_step
    pick = (source == lax.broadcasted_iota(jnp.int32, (total, total), 1)).astype(jnp.bfloat16)
    flat = queries[...].astype(jnp.float32).reshape(total, -1).astype(jnp.bfloat16)
    query = jnp.dot(pick, flat, preferred_element_type=jnp.float32).astype(jnp.bfloat16)
    for g in range(query.shape[1] // HEAD_DIM):
        ordered[g * total : (g + 1) * total, :] = query[:, g * HEAD_DIM : (g + 1) * HEAD_DIM]
    for s in range(seqs):
        own_rows[s * step_rows : (s + 1) * step_rows, :] = decode[s]
    normed = normed_of(own_rows[...], gain[...])
    projected = jnp.dot(normed, weight[...], preferred_element_type=jnp.float32)
    lane = lax.broadcasted_iota(jnp.int32, lengths.shape, 1)
    length = jnp.where(lane == ep * seqs // samples, lengths[...], 0)
    length = jnp.sum(length, axis=1, keepdims=True)
    cosine, sine = angles_of((row_step + length).astype(jnp.float32))
    cosine_out[...] = cosine[own:]
    sine_out[...] = sine[own:]
    keys = turn(projected[:, :HEAD_DIM], cosine[:own], sine[:own])
    own_kv[:, :HEAD_DIM] = keys.astype(jnp.bfloat16)
    own_kv[:, HEAD_DIM:] = projected[:, HEAD_DIM:].astype(jnp.bfloat16)
    key = lax.broadcasted_iota(jnp.int32, (1, eps * here + total), 1)
    key_ep = partner(ep, key // here, eps)
    prompt_ok = (key < eps * here) & (key_ep * here + lax.rem(key, here) < length)
    key_step, key_seq = place(rep, reps, own, step_rows, key - eps * here)
    self_ok = (key >= eps * here) & (key_seq == row_seq) & (key_step <= row_step)
    mask[...] = (prompt_ok | self_ok).astype(jnp.int32)


def ready_part(lengths, gain, weight, decode, queries, here, reps, eps, samples):
    seqs, steps, columns = queries.shape
    total, width = seqs * steps, decode.shape[2]
    own = total // reps
    return pl.pallas_call(
        functools.partial(ready_kernel, reps, eps, here, samples),
        out_shape=[
            on_chip((total * columns // HEAD_DIM, HEAD_DIM), jnp.bfloat16),
            on_chip((total, eps * here + total), jnp.int32),
            on_chip((total - own, HEAD_DIM), jnp.float32),
            on_chip((total - own, HEAD_DIM), jnp.float32),
            on_chip((own, weight.shape[1]), jnp.bfloat16),
            on_chip((own, width), jnp.bfloat16),
        ],
        in_specs=[VMEM] * 5,
        out_specs=[VMEM] * 6,
        compiler_params=pltpu.CompilerParams(vmem_limit_bytes=GRANT),
        cost_estimate=SPAN,
        name="ready_part",
    )(lengths, gain, weight, decode, queries)


def attend_kernel(reps, gain, weight, query, mask, cosine, sine, own_kv, own_rows, out_weight, *rest):
    outs, rows = rest[-reps - 1 : -1], rest[-1]
    others, prompts = rest[: reps - 1], rest[reps - 1 : -reps - 1]
    own, total = own_rows.shape[0], mask.shape[0]
    group = query.shape[0] // total
    seqs, step_rows, _ = others[0].shape
    for k, piece in enumerate(others):
        for s in range(seqs):
            at = k * own + s * step_rows
            rows[at : at + step_rows, :] = piece[s]
    normed = normed_of(rows[...], gain[...])
    projected = jnp.dot(normed, weight[...], preferred_element_type=jnp.float32)
    other_keys = turn(projected[:, :HEAD_DIM], cosine[...], sine[...]).astype(jnp.bfloat16)
    other_values = projected[:, HEAD_DIM:].astype(jnp.bfloat16)
    keys = [p[:, :HEAD_DIM] for p in prompts] + [own_kv[:, :HEAD_DIM], other_keys]
    values = [p[:, HEAD_DIM:] for p in prompts] + [own_kv[:, HEAD_DIM:], other_values]
    keys, values = jnp.concatenate(keys, axis=0), jnp.concatenate(values, axis=0)
    scores = lax.dot_general(
        query[...], keys, (((1,), (1,)), ((), ())), preferred_element_type=jnp.float32
    ) * (HEAD_DIM**-0.5)
    admitted = jnp.concatenate([mask[...]] * group, axis=0) != 0
    scores = jnp.where(admitted, scores, -1e30)
    top = jnp.max(scores, axis=1, keepdims=True)
    weights = jnp.where(admitted, jnp.exp(scores - top), 0.0)
    row_total = jnp.sum(weights, axis=1, keepdims=True)
    weighted = jnp.dot(weights.astype(jnp.bfloat16), values, preferred_element_type=jnp.float32)
    attended = (weighted / row_total).astype(jnp.bfloat16)
    attended = jnp.concatenate(
        [attended[g * total : (g + 1) * total] for g in range(group)], axis=1
    )
    projected = jnp.dot(attended, out_weight[...], preferred_element_type=jnp.float32)
    for k in range(reps):
        part = projected[k * own : (k + 1) * own]
        if k == 0:
            part = part + own_rows[...].astype(jnp.float32)
        outs[k][...] = part.astype(outs[k].dtype)


def attend_part(gain, weight, ready, others, prompts):
    own, width = ready[5].shape
    reps = 1 + len(others)
    shapes = [on_chip((own, width), jnp.float32)]
    shapes += [on_chip((own, width), jnp.bfloat16)] * (reps - 1)
    return pl.pallas_call(
        functools.partial(attend_kernel, reps),
        out_shape=shapes,
        in_specs=[VMEM] * (2 + len(ready) + len(others) + len(prompts)),
        out_specs=[VMEM] * reps,
        scratch_shapes=[pltpu.VMEM(((reps - 1) * own, width), jnp.bfloat16)],
        compiler_params=pltpu.CompilerParams(vmem_limit_bytes=GRANT),
        cost_estimate=SPAN,
        name="attend_part",
    )(gain, weight, *ready, *others, *prompts)


def route_kernel(after, ids, table, pick, pick_back, token_ids, sem):
    del after
    copy = pltpu.make_async_copy(ids, token_ids, sem)
    copy.start()
    step_rows, seqs = token_ids.shape
    count, lanes = seqs * step_rows, table.shape[1]
    lane = lax.broadcasted_iota(jnp.int32, (1, lanes), 1)
    across = jnp.full((1, count), -1, jnp.int32)
    below = jnp.full((count, 1), -1, jnp.int32)
    spot = lax.broadcasted_iota(jnp.int32, (1, count), 1)
    copy.wait()
    for i in range(count):
        token = token_ids[i % step_rows, i // step_rows]
        line = table[pl.ds(token // lanes, 1), :]
        found = jnp.sum(jnp.where(lane == lax.rem(token, lanes), line, 0), axis=1, keepdims=True)
        across = jnp.where(spot == i, found, across)
        below = jnp.where(column(count) == i, found, below)
    same = across == below
    rank = jnp.sum((same & (column(count) < spot)).astype(jnp.int32), axis=0, keepdims=True)
    rank_below = jnp.sum((same & (spot < column(count))).astype(jnp.int32), axis=1, keepdims=True)
    slots = pick.shape[0]
    pick[...] = (column(slots) == across * CAP + rank).astype(jnp.bfloat16)
    slot = lax.broadcasted_iota(jnp.int32, (1, slots), 1)
    pick_back[...] = (slot == below * CAP + rank_below).astype(jnp.bfloat16)


def route_part(after, token_ids, table, slots):
    count = token_ids.size
    token_ids, table = token_ids.T, table.reshape(-1, 128)
    return pl.pallas_call(
        route_kernel,
        out_shape=[
            on_chip((slots, count), jnp.bfloat16),
            on_chip((count, slots), jnp.bfloat16),
        ],
        in_specs=[VMEM, HBM, VMEM],
        out_specs=[VMEM] * 2,
        scratch_shapes=[pltpu.SMEM(token_ids.shape, jnp.int32), pltpu.SemaphoreType.DMA],
        compiler_params=pltpu.CompilerParams(vmem_limit_bytes=GRANT),
        cost_estimate=SPAN,
        name="route_part",
    )(after, *far(token_ids), *held(table))


def send_kernel(gain, pick, own, *rest):
    *others, mixed, outgoing = rest
    total = own[...]
    for piece in others:
        total = total + piece[...].astype(jnp.float32)
    rounded = total.astype(jnp.bfloat16)
    mixed[...] = rounded
    normed = normed_of(rounded, gain[...])
    slots = jnp.dot(pick[...], normed, preferred_element_type=jnp.float32).astype(jnp.bfloat16)
    for d in range(outgoing.shape[0]):
        outgoing[d] = slots[d * CAP : (d + 1) * CAP]


def send_part(gain, pick, shares):
    rows, width = shares[0].shape
    return pl.pallas_call(
        send_kernel,
        out_shape=[
            on_chip((rows, width), jnp.bfloat16),
            on_chip((pick.shape[0] // CAP, CAP, width), jnp.bfloat16),
        ],
        in_specs=[VMEM] * (2 + len(shares)),
        out_specs=[VMEM] * 2,
        compiler_params=pltpu.CompilerParams(vmem_limit_bytes=GRANT),
        name="send_part",
    )(gain, pick, *shares)


def expert_kernel(arrived, gate_weight, up_weight, down_weight, served, rows):
    for d in range(arrived.shape[0]):
        rows[d * CAP : (d + 1) * CAP, :] = arrived[d]
    tokens = rows[...]
    gate_proj = jnp.dot(tokens, gate_weight[0], preferred_element_type=jnp.float32)
    up_proj = jnp.dot(tokens, up_weight[0], preferred_element_type=jnp.float32)
    hidden = (gate_proj / (1.0 + jnp.exp(-gate_proj)) * up_proj).astype(jnp.bfloat16)
    result = jnp.dot(hidden, down_weight[0], preferred_element_type=jnp.float32)
    result = result.astype(jnp.bfloat16)
    for d in range(served.shape[0]):
        served[d] = result[d * CAP : (d + 1) * CAP]


def expert_part(arrived, gate_weight, up_weight, down_weight):
    return pl.pallas_call(
        expert_kernel,
        out_shape=on_chip(arrived.shape, jnp.bfloat16),
        in_specs=[VMEM] * 4,
        out_specs=VMEM,
        scratch_shapes=[pltpu.VMEM((arrived.shape[0] * CAP, arrived.shape[2]), jnp.bfloat16)],
        compiler_params=pltpu.CompilerParams(vmem_limit_bytes=GRANT),
        name="expert_part",
    )(arrived, gate_weight, up_weight, down_weight)


def final_kernel(pick_back, mixed, returned, out, rows):
    for d in range(returned.shape[0]):
        rows[d * CAP : (d + 1) * CAP, :] = returned[d]
    moe_out = jnp.dot(pick_back[...], rows[...], preferred_element_type=jnp.float32)
    total = (mixed[...].astype(jnp.float32) + moe_out).astype(jnp.bfloat16)
    step_rows = out.shape[1]
    for s in range(out.shape[0]):
        out[s] = total[s * step_rows : (s + 1) * step_rows]


def final_part(pick_back, mixed, returned, shape):
    return pl.pallas_call(
        final_kernel,
        out_shape=jax.ShapeDtypeStruct(shape, jnp.bfloat16),
        in_specs=[VMEM] * 3,
        out_specs=VMEM,
        scratch_shapes=[pltpu.VMEM((returned.shape[0] * CAP, returned.shape[2]), jnp.bfloat16)],
        compiler_params=pltpu.CompilerParams(vmem_limit_bytes=GRANT),
        name="final_part",
    )(pick_back, mixed, returned)


def local(
    prompt_hidden,
    decode_hidden,
    queries,
    attn_gain,
    key_value_weight,
    out_weight,
    moe_gain,
    gate_weight,
    up_weight,
    down_weight,
    expert_table,
    token_ids,
    prompt_lengths,
):
    seqs = decode_hidden.shape[0]
    ep_count, rep_count = lax.axis_size("ep"), lax.axis_size("rep")
    samples = seqs * ep_count // GROUP_PROMPTS
    blocks = key_value_weight.shape[1] // HEAD_DIM
    if blocks != 2 or seqs > 8 or samples % seqs or expert_table.shape[0] % 128:
        return general(
            prompt_hidden,
            decode_hidden,
            queries,
            attn_gain,
            key_value_weight,
            out_weight,
            moe_gain,
            gate_weight,
            up_weight,
            down_weight,
            expert_table,
            token_ids,
            prompt_lengths,
        )
    attn_gain, moe_gain = attn_gain[None, :], moe_gain[None, :]
    ahead = ahead_part()
    others = [swap(decode_hidden, "rep", k) for k in range(1, rep_count)]
    gain, weight, own_hidden, query = held(attn_gain, key_value_weight, decode_hidden, queries)
    parts = prompt_part(*held(ahead, prompt_hidden), gain, weight, seqs, samples, ep_count)
    prompts = [swap(part, "ep", k) if k else part for k, part in enumerate(parts)]
    ready = ready_part(
        *held(prompt_lengths[None, :]),
        gain,
        weight,
        own_hidden,
        query,
        prompt_hidden.shape[1],
        rep_count,
        ep_count,
        samples,
    )
    shares = attend_part(
        gain, weight, held(*ready, out_weight), held(*others), held(*prompts)
    )
    pick, pick_back = route_part(
        shares[0], token_ids, expert_table, ep_count * rep_count * CAP
    )
    shares = [swap(share, "rep", k) if k else share for k, share in enumerate(shares)]
    mixed, outgoing = send_part(*held(moe_gain), pick, held(*shares))
    arrived = lax.all_to_all(outgoing, ("ep", "rep"), split_axis=0, concat_axis=0, tiled=True)
    served = expert_part(*held(arrived, gate_weight, up_weight, down_weight))
    returned = lax.all_to_all(served, ("ep", "rep"), split_axis=0, concat_axis=0, tiled=True)
    return final_part(pick_back, mixed, *held(returned), decode_hidden.shape)


def solution(mesh):
    placed = (
        P("groups", "ep", None),
        P(("groups", "ep"), "rep", None),
        P(("groups", "ep"), None, "rep"),
        P(),
        P(None, "rep"),
        P("rep", None),
        P(),
        P(("ep", "rep"), None, None),
        P(("ep", "rep"), None, None),
        P(("ep", "rep"), None, None),
        P(),
        P("ep", "rep"),
        P("groups"),
    )
    return jax.shard_map(
        local,
        mesh=mesh,
        in_specs=placed,
        out_specs=P(("groups", "ep"), "rep", None),
        check_vma=False,
    )
```

```python
import functools
import math

import jax
import jax.numpy as jnp
from jax import lax
from jax.experimental import pallas as pl
from jax.experimental.pallas import tpu as pltpu
from jax.sharding import PartitionSpec as P


HEAD_DIM = 128
GROUP_PROMPTS = 4
CAP = 2

EPS = 1e-06
THETA = 1000000.0


def partner(index, step, count):
    if count & (count - 1) == 0:
        return index ^ step
    return (count + step - index) % count


def swap(block, axis, step):
    count = lax.axis_size(axis)
    return lax.ppermute(block, axis, [(i, partner(i, step, count)) for i in range(count)])


def shifted(block, axis, step, sign):
    count = lax.axis_size(axis)
    route = [(i, (i + sign * step) % count) for i in range(count)]
    return lax.ppermute(block, axis, route)


def normed_of(hidden, gain_vec):
    widened = hidden.astype(jnp.float32)
    mean_sq = jnp.mean(widened * widened, axis=-1, keepdims=True)
    return (widened * lax.rsqrt(mean_sq + EPS) * gain_vec).astype(jnp.bfloat16)


def key_value(hidden, gain_vec, key_value_weight, positions, is_key):
    projected = jnp.dot(
        normed_of(hidden, gain_vec), key_value_weight, preferred_element_type=jnp.float32
    )
    half = HEAD_DIM // 2
    freq = jnp.exp(jnp.arange(half, dtype=jnp.float32) * (-2.0 * math.log(THETA) / HEAD_DIM))
    angles = positions[:, None] * freq
    cosine, sine = jnp.cos(angles), jnp.sin(angles)
    out = []
    for b in range(key_value_weight.shape[1] // HEAD_DIM):
        block = projected[:, b * HEAD_DIM : (b + 1) * HEAD_DIM]
        if is_key[b] is not False:
            first, second = block[:, :half], block[:, half:]
            turned = jnp.concatenate(
                [first * cosine - second * sine, second * cosine + first * sine], axis=1
            )
            block = turned if is_key[b] is True else jnp.where(is_key[b], turned, block)
        out.append(block.astype(jnp.bfloat16))
    return jnp.concatenate(out, axis=1) if len(out) > 1 else out[0]


def general(
    prompt_hidden,
    decode_hidden,
    queries,
    attn_gain,
    key_value_weight,
    out_weight,
    moe_gain,
    gate_weight,
    up_weight,
    down_weight,
    expert_table,
    token_ids,
    prompt_lengths,
):
    seqs, step_rows, model_width = decode_hidden.shape
    prompt_len_local = prompt_hidden.shape[1]
    qh_dev = queries.shape[2] // HEAD_DIM
    ep_count, rep_count = lax.axis_size("ep"), lax.axis_size("rep")
    ep_index, rep_index = lax.axis_index("ep"), lax.axis_index("rep")
    samples = seqs * ep_count // GROUP_PROMPTS
    blocks = key_value_weight.shape[1] // HEAD_DIM
    row_count = seqs * step_rows
    own_prompts = max(1, seqs // samples)

    own_rows = decode_hidden.reshape(row_count, model_width)
    others = [swap(own_rows, "rep", k) for k in range(1, rep_count)]
    owners = [partner(rep_index, k, rep_count) for k in range(rep_count)]

    if blocks == 1:
        is_key = [rep_index % 2 == 0]
    else:
        is_key = [b % 2 == 0 for b in range(blocks)]
    heads_here = max(1, blocks // 2)

    prompt_pos = (
        ep_index * prompt_len_local + jnp.arange(prompt_len_local, dtype=jnp.int32)
    ).astype(jnp.float32)
    prompt_part = key_value(
        prompt_hidden.reshape(-1, model_width),
        attn_gain,
        key_value_weight,
        jnp.tile(prompt_pos, GROUP_PROMPTS),
        is_key,
    ).reshape(GROUP_PROMPTS, prompt_len_local, blocks * HEAD_DIM)

    def first_prompt(ep):
        return ep * seqs // samples

    pieces, piece_pos = [], []
    for k in range(ep_count):
        other = partner(ep_index, k, ep_count)
        part = lax.dynamic_slice_in_dim(prompt_part, first_prompt(other), own_prompts, 0)
        pieces.append(swap(part, "ep", k) if k else part)
        piece_pos.append(other * prompt_len_local + jnp.arange(prompt_len_local, dtype=jnp.int32))
    prompt_kv = jnp.concatenate(pieces, axis=1)
    key_pos = jnp.concatenate(piece_pos)

    own_first = first_prompt(ep_index)
    own_lengths = lax.dynamic_slice_in_dim(prompt_lengths, own_first, own_prompts, 0)
    seq_lengths = jnp.repeat(own_lengths, seqs // own_prompts)

    def decode_part(k):
        step = owners[k] * step_rows + jnp.arange(step_rows, dtype=jnp.int32)
        position = (seq_lengths[:, None] + step[None, :]).astype(jnp.float32).reshape(-1)
        return position

    positions = [decode_part(k) for k in range(rep_count)]
    decode_own = key_value(own_rows, attn_gain, key_value_weight, positions[0], is_key)
    decode_rest = key_value(
        jnp.concatenate(others, axis=0),
        attn_gain,
        key_value_weight,
        jnp.concatenate(positions[1:]),
        is_key,
    )
    decode_kv = jnp.concatenate([decode_own, decode_rest], axis=0)
    if blocks == 1:
        partner_prompt, partner_decode = swap((prompt_kv, decode_kv), "rep", 1)
        holds_key = rep_index % 2 == 0

        def both(mine, theirs):
            return jnp.where(
                holds_key,
                jnp.concatenate([mine, theirs], axis=-1),
                jnp.concatenate([theirs, mine], axis=-1),
            )

        prompt_kv, decode_kv = both(prompt_kv, partner_prompt), both(decode_kv, partner_decode)

    tile = min(seqs // own_prompts, 8)
    tiles = seqs // own_prompts // tile
    group = qh_dev // heads_here
    by_owner = jnp.concatenate(
        [lax.dynamic_slice_in_dim(queries, o * step_rows, step_rows, 1)[None] for o in owners]
    )
    tokens = rep_count * tile * step_rows

    def tiled(rows):
        width = rows.shape[-1]
        rows = rows.reshape(rep_count, own_prompts, tiles, tile * step_rows, width)
        return rows.transpose(1, 2, 0, 3, 4).reshape(own_prompts, tiles, tokens, width)

    query_rows = tiled(by_owner.reshape(rep_count, row_count, qh_dev * HEAD_DIM))
    decode_rows = tiled(decode_kv.reshape(rep_count, row_count, -1))
    row_step = jnp.concatenate(
        [
            jnp.tile(o * step_rows + jnp.arange(step_rows, dtype=jnp.int32), tile)
            for o in owners
        ]
    )
    row_seq = jnp.tile(jnp.repeat(jnp.arange(tile, dtype=jnp.int32), step_rows), rep_count)
    self_mask = (row_seq[:, None] == row_seq[None, :]) & (row_step[None, :] <= row_step[:, None])
    prompt_mask = key_pos[None, :] < own_lengths[:, None]
    score_scale = HEAD_DIM ** (-0.5)

    heads = []
    for h in range(heads_here):
        lo = 2 * h * HEAD_DIM
        prompt_keys = prompt_kv[..., lo : lo + HEAD_DIM]
        prompt_values = prompt_kv[..., lo + HEAD_DIM : lo + 2 * HEAD_DIM]
        self_keys = decode_rows[..., lo : lo + HEAD_DIM]
        self_values = decode_rows[..., lo + HEAD_DIM : lo + 2 * HEAD_DIM]
        query = jnp.stack(
            [
                query_rows[..., (h * group + g) * HEAD_DIM : (h * group + g + 1) * HEAD_DIM]
                for g in range(group)
            ],
            axis=2,
        )
        cache_scores = score_scale * jnp.einsum(
            "pbgrd,pnd->pbgrn", query, prompt_keys, preferred_element_type=jnp.float32
        )
        self_scores = score_scale * jnp.einsum(
            "pbgrd,pbud->pbgru", query, self_keys, preferred_element_type=jnp.float32
        )
        cache_mask = prompt_mask[:, None, None, None, :]
        cache_scores = jnp.where(cache_mask, cache_scores, -1e30)
        self_scores = jnp.where(self_mask, self_scores, -1e30)
        top = jnp.maximum(
            jnp.max(cache_scores, axis=-1, keepdims=True),
            jnp.max(self_scores, axis=-1, keepdims=True),
        )
        cache_weights = jnp.where(cache_mask, jnp.exp(cache_scores - top), 0.0)
        self_weights = jnp.where(self_mask, jnp.exp(self_scores - top), 0.0)
        total = jnp.sum(cache_weights, axis=-1, keepdims=True) + jnp.sum(
            self_weights, axis=-1, keepdims=True
        )
        weighted = jnp.einsum(
            "pbgrn,pnd->pbgrd",
            cache_weights.astype(jnp.bfloat16),
            prompt_values,
            preferred_element_type=jnp.float32,
        ) + jnp.einsum(
            "pbgru,pbud->pbgrd",
            self_weights.astype(jnp.bfloat16),
            self_values,
            preferred_element_type=jnp.float32,
        )
        attended = (weighted / total).astype(jnp.bfloat16)
        heads += [attended[:, :, g] for g in range(group)]
    attended = jnp.concatenate(heads, axis=-1)
    attended = attended.reshape(own_prompts, tiles, rep_count, tile * step_rows, -1)
    attended = attended.transpose(2, 0, 1, 3, 4).reshape(rep_count * row_count, -1)

    projected = (
        jnp.dot(attended, out_weight, preferred_element_type=jnp.float32)
        .astype(jnp.bfloat16)
        .reshape(rep_count, row_count, model_width)
    )
    received = [swap(projected[k], "rep", k) for k in range(1, rep_count)]
    attn_sum = projected[0].astype(jnp.float32)
    for piece in received:
        attn_sum = attn_sum + piece.astype(jnp.float32)
    attn_mixed = (own_rows.astype(jnp.float32) + attn_sum).astype(jnp.bfloat16)

    normed = normed_of(attn_mixed, moe_gain)
    chosen = jnp.take(expert_table, token_ids.reshape(row_count))
    device_count = ep_count * rep_count
    slot_total = device_count * CAP
    same_expert = chosen[:, None] == chosen[None, :]
    before = jnp.arange(row_count)[None, :] < jnp.arange(row_count)[:, None]
    slot_rank = jnp.sum((same_expert & before).astype(jnp.int32), axis=1)
    destination = chosen * CAP + slot_rank
    send_pick = (jnp.arange(slot_total, dtype=jnp.int32)[:, None] == destination[None, :]).astype(
        jnp.bfloat16
    )
    outgoing = (
        jnp.dot(send_pick, normed, preferred_element_type=jnp.float32)
        .astype(jnp.bfloat16)
        .reshape(device_count, CAP, model_width)
    )
    arrived = lax.all_to_all(outgoing, ("ep", "rep"), split_axis=0, concat_axis=0, tiled=True)
    flat_rows = arrived.reshape(slot_total, model_width)
    gate_proj = jnp.dot(flat_rows, gate_weight[0], preferred_element_type=jnp.float32)
    up_proj = jnp.dot(flat_rows, up_weight[0], preferred_element_type=jnp.float32)
    hidden = (jax.nn.silu(gate_proj) * up_proj).astype(jnp.bfloat16)
    served = (
        jnp.dot(hidden, down_weight[0], preferred_element_type=jnp.float32)
        .astype(jnp.bfloat16)
        .reshape(device_count, CAP, model_width)
    )
    returned = lax.all_to_all(served, ("ep", "rep"), split_axis=0, concat_axis=0, tiled=True)
    moe_out = lax.dot_general(
        send_pick,
        returned.reshape(slot_total, model_width),
        (((0,), (0,)), ((), ())),
        preferred_element_type=jnp.float32,
    )
    layer_out = (attn_mixed.astype(jnp.float32) + moe_out).astype(jnp.bfloat16)
    return layer_out.reshape(seqs, step_rows, model_width)


GRANT = 16 << 20
SPAN = pl.CostEstimate(flops=1 << 32, transcendentals=0, bytes_accessed=1 << 20)
VMEM = pl.BlockSpec(memory_space=pltpu.VMEM)


def on_chip(shape, dtype):
    return pltpu.VMEM(shape, dtype)


def far(*arrays):
    return [pltpu.with_memory_space_constraint(a, pltpu.HBM) for a in arrays]


def held(*arrays):
    return [pltpu.with_memory_space_constraint(a, pltpu.VMEM) for a in arrays]


def angles_of(positions):
    half = HEAD_DIM // 2
    lane = lax.broadcasted_iota(jnp.int32, (1, HEAD_DIM), 1)
    spot = jnp.where(lane < half, lane, lane - half).astype(jnp.float32)
    angles = positions * jnp.exp(spot * (-2.0 * math.log(THETA) / HEAD_DIM))
    sine = jnp.sin(angles)
    return jnp.cos(angles), jnp.where(lane < half, -sine, sine)


def turn(block, cosine, sine):
    return block * cosine + pltpu.roll(block, HEAD_DIM // 2, 1) * sine


def column(count):
    return lax.broadcasted_iota(jnp.int32, (count, 1), 0)


HBM = pl.BlockSpec(memory_space=pltpu.HBM)


def ahead_kernel(out):
    out[...] = jnp.zeros(out.shape, out.dtype)


def ahead_part():
    return pl.pallas_call(
        ahead_kernel,
        out_shape=on_chip((8, HEAD_DIM), jnp.float32),
        out_specs=VMEM,
        compiler_params=pltpu.CompilerParams(vmem_limit_bytes=GRANT),
        cost_estimate=SPAN,
        name="ahead_part",
    )()


def prompt_kernel(seqs, samples, ahead, hidden, gain, weight, *rest):
    del ahead
    *outs, scratch = rest
    prompts, here, width = hidden.shape
    ep = lax.axis_index("ep")
    spot = lax.rem(column(prompts * here), here) + ep * here
    cosine, sine = angles_of(spot.astype(jnp.float32))
    normed = normed_of(hidden[...].astype(jnp.float32).reshape(prompts * here, width), gain[...])
    projected = jnp.dot(normed, weight[...], preferred_element_type=jnp.float32)
    keys = turn(projected[:, :HEAD_DIM], cosine, sine)
    scratch[:, :, :HEAD_DIM] = keys.reshape(prompts, here, HEAD_DIM)
    scratch[:, :, HEAD_DIM:] = projected[:, HEAD_DIM:].reshape(prompts, here, HEAD_DIM)
    for k, out in enumerate(outs):
        first = partner(ep, k, len(outs)) * seqs // samples
        out[...] = scratch[first].astype(jnp.bfloat16)


def prompt_part(ahead, prompt_hidden, gain, weight, seqs, samples, ep_count):
    prompts, here, _ = prompt_hidden.shape
    columns = weight.shape[1]
    return pl.pallas_call(
        functools.partial(prompt_kernel, seqs, samples),
        out_shape=[on_chip((here, columns), jnp.bfloat16)] * ep_count,
        in_specs=[VMEM] * 4,
        out_specs=[VMEM] * ep_count,
        scratch_shapes=[pltpu.VMEM((prompts, here, columns), jnp.float32)],
        compiler_params=pltpu.CompilerParams(vmem_limit_bytes=GRANT),
        cost_estimate=SPAN,
        name="prompt_part",
    )(ahead, prompt_hidden, gain, weight)


def place(rep, reps, own, step_rows, index):
    k = index // own
    sequence = lax.rem(index, own) // step_rows
    return lax.rem(rep + reps - k, reps) * step_rows + lax.rem(index, step_rows), sequence


def ready_kernel(reps, eps, here, samples, lengths, gain, weight, decode, queries, *rest):
    ordered, mask, cosine_out, sine_out, own_kv, own_rows = rest
    seqs, steps, _ = queries.shape
    step_rows = steps // reps
    own = seqs * step_rows
    total = reps * own
    ep, rep = lax.axis_index("ep"), lax.axis_index("rep")
    row_step, row_seq = place(rep, reps, own, step_rows, column(total))
    source = row_seq * steps + row_step
    pick = (source == lax.broadcasted_iota(jnp.int32, (total, total), 1)).astype(jnp.bfloat16)
    flat = queries[...].astype(jnp.float32).reshape(total, -1).astype(jnp.bfloat16)
    query = jnp.dot(pick, flat, preferred_element_type=jnp.float32).astype(jnp.bfloat16)
    for g in range(query.shape[1] // HEAD_DIM):
        ordered[g * total : (g + 1) * total, :] = query[:, g * HEAD_DIM : (g + 1) * HEAD_DIM]
    for s in range(seqs):
        own_rows[s * step_rows : (s + 1) * step_rows, :] = decode[s]
    normed = normed_of(own_rows[...], gain[...])
    projected = jnp.dot(normed, weight[...], preferred_element_type=jnp.float32)
    lane = lax.broadcasted_iota(jnp.int32, lengths.shape, 1)
    length = jnp.where(lane == ep * seqs // samples, lengths[...], 0)
    length = jnp.sum(length, axis=1, keepdims=True)
    cosine, sine = angles_of((row_step + length).astype(jnp.float32))
    cosine_out[...] = cosine[own:]
    sine_out[...] = sine[own:]
    keys = turn(projected[:, :HEAD_DIM], cosine[:own], sine[:own])
    own_kv[:, :HEAD_DIM] = keys.astype(jnp.bfloat16)
    own_kv[:, HEAD_DIM:] = projected[:, HEAD_DIM:].astype(jnp.bfloat16)
    key = lax.broadcasted_iota(jnp.int32, (1, eps * here + total), 1)
    key_ep = partner(ep, key // here, eps)
    prompt_ok = (key < eps * here) & (key_ep * here + lax.rem(key, here) < length)
    key_step, key_seq = place(rep, reps, own, step_rows, key - eps * here)
    self_ok = (key >= eps * here) & (key_seq == row_seq) & (key_step <= row_step)
    mask[...] = (prompt_ok | self_ok).astype(jnp.int32)


def ready_part(lengths, gain, weight, decode, queries, here, reps, eps, samples):
    seqs, steps, columns = queries.shape
    total, width = seqs * steps, decode.shape[2]
    own = total // reps
    return pl.pallas_call(
        functools.partial(ready_kernel, reps, eps, here, samples),
        out_shape=[
            on_chip((total * columns // HEAD_DIM, HEAD_DIM), jnp.bfloat16),
            on_chip((total, eps * here + total), jnp.int32),
            on_chip((total - own, HEAD_DIM), jnp.float32),
            on_chip((total - own, HEAD_DIM), jnp.float32),
            on_chip((own, weight.shape[1]), jnp.bfloat16),
            on_chip((own, width), jnp.bfloat16),
        ],
        in_specs=[VMEM] * 5,
        out_specs=[VMEM] * 6,
        compiler_params=pltpu.CompilerParams(vmem_limit_bytes=GRANT),
        cost_estimate=SPAN,
        name="ready_part",
    )(lengths, gain, weight, decode, queries)


def attend_kernel(reps, gain, weight, query, mask, cosine, sine, own_kv, own_rows, out_weight, *rest):
    outs, rows = rest[-reps - 1 : -1], rest[-1]
    others, prompts = rest[: reps - 1], rest[reps - 1 : -reps - 1]
    own, total = own_rows.shape[0], mask.shape[0]
    group = query.shape[0] // total
    seqs, step_rows, _ = others[0].shape
    for k, piece in enumerate(others):
        for s in range(seqs):
            at = k * own + s * step_rows
            rows[at : at + step_rows, :] = piece[s]
    normed = normed_of(rows[...], gain[...])
    projected = jnp.dot(normed, weight[...], preferred_element_type=jnp.float32)
    other_keys = turn(projected[:, :HEAD_DIM], cosine[...], sine[...]).astype(jnp.bfloat16)
    other_values = projected[:, HEAD_DIM:].astype(jnp.bfloat16)
    keys = [p[:, :HEAD_DIM] for p in prompts] + [own_kv[:, :HEAD_DIM], other_keys]
    values = [p[:, HEAD_DIM:] for p in prompts] + [own_kv[:, HEAD_DIM:], other_values]
    keys, values = jnp.concatenate(keys, axis=0), jnp.concatenate(values, axis=0)
    scores = lax.dot_general(
        query[...], keys, (((1,), (1,)), ((), ())), preferred_element_type=jnp.float32
    ) * (HEAD_DIM**-0.5)
    admitted = jnp.concatenate([mask[...]] * group, axis=0) != 0
    scores = jnp.where(admitted, scores, -1e30)
    top = jnp.max(scores, axis=1, keepdims=True)
    weights = jnp.where(admitted, jnp.exp(scores - top), 0.0)
    row_total = jnp.sum(weights, axis=1, keepdims=True)
    weighted = jnp.dot(weights.astype(jnp.bfloat16), values, preferred_element_type=jnp.float32)
    attended = (weighted / row_total).astype(jnp.bfloat16)
    attended = jnp.concatenate(
        [attended[g * total : (g + 1) * total] for g in range(group)], axis=1
    )
    projected = jnp.dot(attended, out_weight[...], preferred_element_type=jnp.float32)
    for k in range(reps):
        part = projected[k * own : (k + 1) * own]
        if k == 0:
            part = part + own_rows[...].astype(jnp.float32)
        outs[k][...] = part.astype(outs[k].dtype)


def attend_part(gain, weight, ready, others, prompts):
    own, width = ready[5].shape
    reps = 1 + len(others)
    shapes = [on_chip((own, width), jnp.float32)]
    shapes += [on_chip((own, width), jnp.bfloat16)] * (reps - 1)
    return pl.pallas_call(
        functools.partial(attend_kernel, reps),
        out_shape=shapes,
        in_specs=[VMEM] * (2 + len(ready) + len(others) + len(prompts)),
        out_specs=[VMEM] * reps,
        scratch_shapes=[pltpu.VMEM(((reps - 1) * own, width), jnp.bfloat16)],
        compiler_params=pltpu.CompilerParams(vmem_limit_bytes=GRANT),
        cost_estimate=SPAN,
        name="attend_part",
    )(gain, weight, *ready, *others, *prompts)


def route_kernel(after, ids, table, pick, pick_back, token_ids, sem):
    del after
    copy = pltpu.make_async_copy(ids, token_ids, sem)
    copy.start()
    step_rows, seqs = token_ids.shape
    count, lanes = seqs * step_rows, table.shape[1]
    lane = lax.broadcasted_iota(jnp.int32, (1, lanes), 1)
    across = jnp.full((1, count), -1, jnp.int32)
    below = jnp.full((count, 1), -1, jnp.int32)
    spot = lax.broadcasted_iota(jnp.int32, (1, count), 1)
    copy.wait()
    for i in range(count):
        token = token_ids[i % step_rows, i // step_rows]
        line = table[pl.ds(token // lanes, 1), :]
        found = jnp.sum(jnp.where(lane == lax.rem(token, lanes), line, 0), axis=1, keepdims=True)
        across = jnp.where(spot == i, found, across)
        below = jnp.where(column(count) == i, found, below)
    same = across == below
    rank = jnp.sum((same & (column(count) < spot)).astype(jnp.int32), axis=0, keepdims=True)
    rank_below = jnp.sum((same & (spot < column(count))).astype(jnp.int32), axis=1, keepdims=True)
    slots = pick.shape[0]
    pick[...] = (column(slots) == across * CAP + rank).astype(jnp.bfloat16)
    slot = lax.broadcasted_iota(jnp.int32, (1, slots), 1)
    pick_back[...] = (slot == below * CAP + rank_below).astype(jnp.bfloat16)


def route_part(after, token_ids, table, slots):
    count = token_ids.size
    token_ids, table = token_ids.T, table.reshape(-1, 128)
    return pl.pallas_call(
        route_kernel,
        out_shape=[
            on_chip((slots, count), jnp.bfloat16),
            on_chip((count, slots), jnp.bfloat16),
        ],
        in_specs=[VMEM, HBM, VMEM],
        out_specs=[VMEM] * 2,
        scratch_shapes=[pltpu.SMEM(token_ids.shape, jnp.int32), pltpu.SemaphoreType.DMA],
        compiler_params=pltpu.CompilerParams(vmem_limit_bytes=GRANT),
        cost_estimate=SPAN,
        name="route_part",
    )(after, *far(token_ids), *held(table))


def send_kernel(gain, pick, own, *rest):
    *others, mixed, outgoing = rest
    total = own[...]
    for piece in others:
        total = total + piece[...].astype(jnp.float32)
    rounded = total.astype(jnp.bfloat16)
    mixed[...] = rounded
    normed = normed_of(rounded, gain[...])
    slots = jnp.dot(pick[...], normed, preferred_element_type=jnp.float32).astype(jnp.bfloat16)
    for d in range(outgoing.shape[0]):
        outgoing[d] = slots[d * CAP : (d + 1) * CAP]


def send_part(gain, pick, shares):
    rows, width = shares[0].shape
    return pl.pallas_call(
        send_kernel,
        out_shape=[
            on_chip((rows, width), jnp.bfloat16),
            on_chip((pick.shape[0] // CAP, CAP, width), jnp.bfloat16),
        ],
        in_specs=[VMEM] * (2 + len(shares)),
        out_specs=[VMEM] * 2,
        compiler_params=pltpu.CompilerParams(vmem_limit_bytes=GRANT),
        name="send_part",
    )(gain, pick, *shares)


def expert_kernel(arrived, gate_weight, up_weight, down_weight, served, rows):
    for d in range(arrived.shape[0]):
        rows[d * CAP : (d + 1) * CAP, :] = arrived[d]
    tokens = rows[...]
    gate_proj = jnp.dot(tokens, gate_weight[0], preferred_element_type=jnp.float32)
    up_proj = jnp.dot(tokens, up_weight[0], preferred_element_type=jnp.float32)
    hidden = (gate_proj / (1.0 + jnp.exp(-gate_proj)) * up_proj).astype(jnp.bfloat16)
    result = jnp.dot(hidden, down_weight[0], preferred_element_type=jnp.float32)
    result = result.astype(jnp.bfloat16)
    for d in range(served.shape[0]):
        served[d] = result[d * CAP : (d + 1) * CAP]


def expert_part(arrived, gate_weight, up_weight, down_weight):
    return pl.pallas_call(
        expert_kernel,
        out_shape=on_chip(arrived.shape, jnp.bfloat16),
        in_specs=[VMEM] * 4,
        out_specs=VMEM,
        scratch_shapes=[pltpu.VMEM((arrived.shape[0] * CAP, arrived.shape[2]), jnp.bfloat16)],
        compiler_params=pltpu.CompilerParams(vmem_limit_bytes=GRANT),
        name="expert_part",
    )(arrived, gate_weight, up_weight, down_weight)


def final_kernel(pick_back, mixed, returned, out, rows):
    for d in range(returned.shape[0]):
        rows[d * CAP : (d + 1) * CAP, :] = returned[d]
    moe_out = jnp.dot(pick_back[...], rows[...], preferred_element_type=jnp.float32)
    total = (mixed[...].astype(jnp.float32) + moe_out).astype(jnp.bfloat16)
    step_rows = out.shape[1]
    for s in range(out.shape[0]):
        out[s] = total[s * step_rows : (s + 1) * step_rows]


def final_part(pick_back, mixed, returned, shape):
    return pl.pallas_call(
        final_kernel,
        out_shape=jax.ShapeDtypeStruct(shape, jnp.bfloat16),
        in_specs=[VMEM] * 3,
        out_specs=VMEM,
        scratch_shapes=[pltpu.VMEM((returned.shape[0] * CAP, returned.shape[2]), jnp.bfloat16)],
        compiler_params=pltpu.CompilerParams(vmem_limit_bytes=GRANT),
        name="final_part",
    )(pick_back, mixed, returned)


def local(
    prompt_hidden,
    decode_hidden,
    queries,
    attn_gain,
    key_value_weight,
    out_weight,
    moe_gain,
    gate_weight,
    up_weight,
    down_weight,
    expert_table,
    token_ids,
    prompt_lengths,
):
    seqs = decode_hidden.shape[0]
    ep_count, rep_count = lax.axis_size("ep"), lax.axis_size("rep")
    samples = seqs * ep_count // GROUP_PROMPTS
    blocks = key_value_weight.shape[1] // HEAD_DIM
    if blocks != 2 or seqs > 8 or samples % seqs or expert_table.shape[0] % 128:
        return general(
            prompt_hidden,
            decode_hidden,
            queries,
            attn_gain,
            key_value_weight,
            out_weight,
            moe_gain,
            gate_weight,
            up_weight,
            down_weight,
            expert_table,
            token_ids,
            prompt_lengths,
        )
    attn_gain, moe_gain = attn_gain[None, :], moe_gain[None, :]
    ahead = ahead_part()
    others = [shifted(decode_hidden, "rep", k, 1) for k in range(1, rep_count)]
    gain, weight, own_hidden, query = held(attn_gain, key_value_weight, decode_hidden, queries)
    parts = prompt_part(*held(ahead, prompt_hidden), gain, weight, seqs, samples, ep_count)
    prompts = [swap(part, "ep", k) if k else part for k, part in enumerate(parts)]
    ready = ready_part(
        *held(prompt_lengths[None, :]),
        gain,
        weight,
        own_hidden,
        query,
        prompt_hidden.shape[1],
        rep_count,
        ep_count,
        samples,
    )
    shares = attend_part(
        gain, weight, held(*ready, out_weight), held(*others), held(*prompts)
    )
    pick, pick_back = route_part(
        shares[0], token_ids, expert_table, ep_count * rep_count * CAP
    )
    shares = [shifted(share, "rep", k, -1) if k else share for k, share in enumerate(shares)]
    mixed, outgoing = send_part(*held(moe_gain), pick, held(*shares))
    arrived = lax.all_to_all(outgoing, ("ep", "rep"), split_axis=0, concat_axis=0, tiled=True)
    served = expert_part(*held(arrived, gate_weight, up_weight, down_weight))
    returned = lax.all_to_all(served, ("ep", "rep"), split_axis=0, concat_axis=0, tiled=True)
    return final_part(pick_back, mixed, *held(returned), decode_hidden.shape)


def solution(mesh):
    placed = (
        P("groups", "ep", None),
        P(("groups", "ep"), "rep", None),
        P(("groups", "ep"), None, "rep"),
        P(),
        P(None, "rep"),
        P("rep", None),
        P(),
        P(("ep", "rep"), None, None),
        P(("ep", "rep"), None, None),
        P(("ep", "rep"), None, None),
        P(),
        P("ep", "rep"),
        P("groups"),
    )
    return jax.shard_map(
        local,
        mesh=mesh,
        in_specs=placed,
        out_specs=P(("groups", "ep"), "rep", None),
        check_vma=False,
    )
```
